256 devices in a mesh: groups: 4 (over y, x), expert: 64 (over z, core).
Axes of the slice: x: 2, y: 2, z: 32, core: 2. Of those that a mesh axis runs over, the one named last changes fastest.
The devices are a block of a 4x8x32 slice.
Arguments:
- queries: bfloat16 [2048, 4096], P(('groups', 'expert')), parts along dimension 0, may hold values from -150 to 150
- key_cache: bfloat16 [2048, 64, 512], P(('groups', 'expert')), parts along dimension 0, may hold values from -7 to 7
- value_cache: bfloat16 [2048, 64, 512], P(('groups', 'expert')), parts along dimension 0, may hold values from -6 to 6
- new_key: bfloat16 [2048, 512], P(('groups', 'expert')), parts along dimension 0, may hold values from -6 to 6
- new_value: bfloat16 [2048, 512], P(('groups', 'expert')), parts along dimension 0, may hold values from -6 to 6
- cache_lengths: int32 [2048], P(('groups', 'expert')), parts along dimension 0, may hold values from 2 to 64, as said below
- hidden_in: bfloat16 [16384, 2048], P(('groups', 'expert')), parts along dimension 0, may hold values from -6 to 6
- norm_gain: bfloat16 [2048], replicated, may hold values from 0.5 to 1.5
- router_weight: bfloat16 [2048, 64], replicated, may hold values from -0.125 to 0.125
- expert_ids: int32 [16384, 8], P(('groups', 'expert')), parts along dimension 0, may hold values from 0 to 63, all different within a row; in each aligned block of 64 rows (0 to 63, 64 to 127, ...) at most 16 rows name the same one
- gate_train: bfloat16 [64, 2048, 768], P(None, 'expert'), may hold values from -0.125 to 0.125
- up_train: bfloat16 [64, 2048, 768], P(None, 'expert'), may hold values from -0.125 to 0.125
- down_train: bfloat16 [64, 768, 2048], P(None, 'expert'), may hold values from -0.21875 to 0.21875
Outputs:
- attended: bfloat16 [2048, 4096], P(('groups', 'expert')), parts along dimension 0
- expert_mix: bfloat16 [16384, 2048], P(('groups', 'expert')), parts along dimension 0
The draws below stay inside these ranges and needn't reach their ends.
There are 4 independent parts, one for each index of `groups`. The reference program is written for one: setup_inputs(seed, part) draws one part's arguments, and reference() takes and returns one part's arrays. A program takes and returns all parts, laid end to end along the dimension named above; an argument that names none is the same for every part. Nothing has to cross between parts.
Inputs may be any that keep to these rules, and one draw needn't show every extreme that they name: `expert_ids`: each row names 8 different experts; within the rows of one device no expert is named more than 16 times. `cache_lengths`: the first sequence of each device's 8 has all 64 positions filled.
All inputs are finite; a program needn't handle non-finite values.
Results may differ from the reference program's by a relative error of at most 0.0074.
Values may be sent and summed in bfloat16 or wider, within the bound.
A program may use at most 128 MiB of HBM per device.

```python
import math
import jax
import jax.numpy as jnp
import numpy as np
from jax import lax

D = 2048
FF = 768
HEADS = 32
KV_HEADS = 4
HEAD_DIM = 128
TOP = 8
TOK_DEV = 64
ATT_DEV = 8
CTX = 64
EXPERTS = 64
TOKENS = 4096
SEQS = 512
CAP = 16
N_EXPERT = 64


def cache_base(key):
    return jnp.clip(jax.random.normal(jax.random.fold_in(key, 7), (SEQS, CTX, KV_HEADS * HEAD_DIM), jnp.float32), -6.0, 6.0)


def draw_key_cache(key, part):
    values = cache_base(key)
    return values.astype(jnp.bfloat16)


def draw_queries(key, part):
    values = jnp.clip(jax.random.normal(jax.random.fold_in(key, 9), (SEQS, HEADS * HEAD_DIM), jnp.float32), -6.0, 6.0)
    return values.astype(jnp.bfloat16)


def draw_cache_lengths(key, part):
    lengths = jax.random.randint(jax.random.fold_in(key, 12), (SEQS,), 2, CTX + 1, jnp.int32)
    return lengths.at[::ATT_DEV].set(CTX)


def levels(rng, shape, shards, low, top_value):
    loudness, own = 1.0, jax.random.fold_in(rng, 6)
    for dim, blocks in shards:
        heights = jnp.exp(jax.random.uniform(jax.random.fold_in(own, dim), (blocks,), jnp.float32, low / len(shards), top_value / len(shards)))
        loudness = loudness * jnp.repeat(heights, shape[dim] // blocks).reshape([-1 if axis == dim else 1 for axis in range(len(shape))])
    return loudness


def shared_out(key, own, number, rows, amount, top, bound, slope):
    order = jax.random.permutation(key, amount)
    heavy_load, common = shares(amount, rows * top, bound, slope, True), shares(amount, rows * top, bound, slope, False)
    places = jnp.arange(amount)

    def named(sizes, offset_by):
        used = int((sizes > 0).sum())
        fixed = max(1, used // 4)
        moved = fixed + (places - fixed + offset_by * (used - fixed)) % max(1, amount - fixed)
        return jnp.zeros((amount,), jnp.int32).at[order[jnp.where(places < fixed, places, moved)]].set(jnp.asarray(sizes, jnp.int32))

    sizes = jnp.where(number % 4 == 0, named(heavy_load, number // 4), named(common, number - number // 4 - 1))
    mixed = jax.random.permutation(jax.random.fold_in(own, 3), amount)
    giver, taker = mixed[0:amount // 2 * 2:2], mixed[1:amount // 2 * 2:2]
    margin = jnp.minimum(sizes[giver] - 1, bound - sizes[taker]) // 2
    margin = jnp.where((giver == order[0]) | (taker == order[0]) | (sizes[taker] == 0), 0, jnp.maximum(margin, 0))
    moved = jax.random.randint(jax.random.fold_in(own, 4), (amount // 2,), 0, 1 << 20) % (margin + 1)
    sizes = sizes.at[giver].add(-moved).at[taker].add(moved)
    labels = jnp.searchsorted(jnp.cumsum(sizes), jnp.arange(rows * top), side="right").astype(jnp.int32)
    listing = labels.reshape(top, rows).T
    listing = listing[jax.random.permutation(jax.random.fold_in(own, 1), rows)]
    offset_by = jax.random.randint(jax.random.fold_in(own, 2), (rows, 1), 0, top)
    return jnp.take_along_axis(listing, (jnp.arange(top)[None, :] + offset_by) % top, axis=1)


def shares(amount, total, reach, slope, full):
    loads = [(1 << 20) // math.isqrt(rank ** slope) + 1 for rank in range(1, amount + 1)]
    largest = reach if full else min(reach, max(-(-total // amount), total * loads[0] // sum(loads)))
    least = 1 if total - largest >= amount - 1 else 0
    holding, spare = [largest] + [least] * (amount - 1), total - largest - least * (amount - 1)
    while spare > 0:
        movable = [i for i in range(1, amount) if holding[i] < largest] or [i for i in range(1, amount) if holding[i] < reach]
        whole, left = sum([loads[i] for i in movable]), spare
        for i in movable:
            addition = min(reach - holding[i], max(1, left * loads[i] // whole), spare)
            holding[i] = holding[i] + addition
            spare = spare - addition
    return np.array(holding)


def centred(key, dims, width, limit, cuts=(), kind=jnp.bfloat16):
    result = width * jax.random.normal(key, dims, jnp.float32)
    if cuts:
        result = result * levels(key, dims, cuts, -0.22, 0.18)
    return jnp.clip(result, -limit, limit).astype(kind)


def setup_inputs(seed: int = 0, part: int = 0) -> dict:
    keys = jax.random.split(jax.random.key(seed), 14)
    part_keys = jax.random.split(jax.random.fold_in(keys[13], part), 14)
    queries = draw_queries(jax.random.fold_in(jax.random.fold_in(keys[13], part), 71), part)
    key_cache = draw_key_cache(jax.random.fold_in(jax.random.fold_in(keys[13], part), 71), part)
    value_cache = centred(part_keys[2], (SEQS, CTX, KV_HEADS * HEAD_DIM), 1.0, 6.0, ((0, 64),))
    new_key = centred(part_keys[3], (SEQS, KV_HEADS * HEAD_DIM), 1.0, 6.0, ((0, 64),))
    new_value = centred(part_keys[4], (SEQS, KV_HEADS * HEAD_DIM), 1.0, 6.0, ((0, 64),))
    cache_lengths = draw_cache_lengths(jax.random.fold_in(jax.random.fold_in(keys[13], part), 71), part)
    hidden_in = centred(part_keys[6], (TOKENS, D), 1.0, 6.0, ((0, 64),))
    norm_gain = jnp.clip(1.0 + 0.1 * jax.random.normal(keys[7], (D,), jnp.float32), 0.5, 1.5).astype(jnp.bfloat16)
    router_weight = centred(keys[8], (D, EXPERTS), D ** -0.5, 0.125)
    expert_ids_keys = jax.random.split(jax.random.fold_in(part_keys[9], 1), TOKENS // TOK_DEV)
    expert_ids_turns = jax.random.permutation(jax.random.fold_in(part_keys[9], 3), TOKENS // TOK_DEV)
    expert_ids = jax.vmap(lambda own, number: shared_out(jax.random.fold_in(part_keys[9], 2), own, number, TOK_DEV, EXPERTS, TOP, CAP, 1))(expert_ids_keys, expert_ids_turns).reshape((TOKENS, TOP))
    gate_train = centred(keys[10], (EXPERTS, D, FF), D ** -0.5, 0.125, ((1, 64),))
    up_train = centred(keys[11], (EXPERTS, D, FF), D ** -0.5, 0.125, ((1, 64),))
    down_train = centred(keys[12], (EXPERTS, FF, D), FF ** -0.5, 0.21875, ((1, 64),))
    return dict(queries=queries, key_cache=key_cache, value_cache=value_cache, new_key=new_key, new_value=new_value, cache_lengths=cache_lengths, hidden_in=hidden_in, norm_gain=norm_gain, router_weight=router_weight, expert_ids=expert_ids, gate_train=gate_train, up_train=up_train, down_train=down_train)


EPSILON = 1e-06

def rms_normed(hidden_in, norm_gain):
    values = hidden_in.astype(jnp.float32)
    mean_square = lax.optimization_barrier(jnp.mean(values * values, axis=-1, keepdims=True))
    return (values * lax.rsqrt(mean_square + EPSILON) * norm_gain.astype(jnp.float32)).astype(jnp.bfloat16)

def attend(queries, key_cache, value_cache, new_key, new_value, cache_lengths):
    seq_count = queries.shape[0]
    group_size = HEADS // KV_HEADS
    query_blocks = queries.astype(jnp.float32).reshape(seq_count, KV_HEADS, group_size, HEAD_DIM)
    cached_keys = key_cache.astype(jnp.float32).reshape(seq_count, CTX, KV_HEADS, HEAD_DIM)
    cached_values = value_cache.astype(jnp.float32).reshape(seq_count, CTX, KV_HEADS, HEAD_DIM)
    fresh_keys = new_key.astype(jnp.float32).reshape(seq_count, KV_HEADS, HEAD_DIM)
    fresh_values = new_value.astype(jnp.float32).reshape(seq_count, KV_HEADS, HEAD_DIM)
    score_scale = 1.0 / math.sqrt(HEAD_DIM)
    scores = jnp.einsum('sgrd,scgd->sgrc', query_blocks, cached_keys) * score_scale
    own_score = jnp.einsum('sgrd,sgd->sgr', query_blocks, fresh_keys) * score_scale
    positions = jnp.arange(CTX, dtype=jnp.int32)
    visible = positions[None, :] < cache_lengths.astype(jnp.int32)[:, None]
    scores = jnp.where(visible[:, None, None, :], scores, -1e+30)
    largest = jnp.maximum(lax.optimization_barrier(jnp.max(scores, axis=-1)), own_score)
    cached_exp = jnp.exp(scores - largest[..., None])
    own_exp = jnp.exp(own_score - largest)
    prob_total = lax.optimization_barrier(jnp.sum(cached_exp, axis=-1)) + own_exp
    cached_prob = lax.optimization_barrier((cached_exp / prob_total[..., None]).astype(jnp.bfloat16)).astype(jnp.float32)
    own_prob = lax.optimization_barrier((own_exp / prob_total).astype(jnp.bfloat16)).astype(jnp.float32)
    context = jnp.einsum('sgrc,scgd->sgrd', cached_prob, cached_values)
    context = context + own_prob[..., None] * fresh_values[:, :, None, :]
    return context.reshape(seq_count, HEADS * HEAD_DIM).astype(jnp.bfloat16)

def expert_block(operands):
    token_rows, gate_weight, up_weight, down_weight = operands
    gate_proj = jnp.dot(token_rows, gate_weight, preferred_element_type=jnp.float32)
    up_proj = jnp.dot(token_rows, up_weight, preferred_element_type=jnp.float32)
    hidden_units = (jax.nn.silu(gate_proj) * up_proj).astype(jnp.bfloat16)
    return jnp.dot(hidden_units, down_weight, preferred_element_type=jnp.float32).astype(jnp.bfloat16)

def mix_experts(hidden_in, norm_gain, router_weight, expert_ids, gate_train, up_train, down_train):
    normed = rms_normed(hidden_in, norm_gain)
    logits = jnp.dot(normed, router_weight, preferred_element_type=jnp.float32)
    expert_range = jnp.arange(EXPERTS, dtype=jnp.int32)
    picked = expert_ids.astype(jnp.int32)[:, :, None] == expert_range[None, None, :]
    chosen = lax.optimization_barrier(jnp.sum(jnp.where(picked, logits[:, None, :], 0.0), axis=-1))
    mixing = jax.nn.softmax(chosen, axis=-1)
    onehot_int = picked.astype(jnp.int32).reshape(N_EXPERT, TOK_DEV * TOP, EXPERTS)
    rank_values = lax.optimization_barrier(jnp.sum((jnp.cumsum(onehot_int, axis=1).astype(jnp.int32) - 1) * onehot_int, axis=-1)).astype(jnp.int32)
    sources = jnp.arange(N_EXPERT, dtype=jnp.int32)[:, None]
    slot_index = (sources * CAP + rank_values).reshape(-1).astype(jnp.int32)
    flat_ids = expert_ids.reshape(-1).astype(jnp.int32)
    repeated = jnp.repeat(normed, TOP, axis=0)
    buffers = jnp.zeros((EXPERTS, N_EXPERT * CAP, D), jnp.bfloat16).at[flat_ids, slot_index].set(repeated)
    outputs = lax.map(expert_block, (buffers, gate_train, up_train, down_train))
    returned = outputs[flat_ids, slot_index].astype(jnp.float32).reshape(TOKENS, TOP, D)
    return lax.optimization_barrier(jnp.sum(mixing[:, :, None] * returned, axis=1)).astype(jnp.bfloat16)

def reference(queries, key_cache, value_cache, new_key, new_value, cache_lengths, hidden_in, norm_gain, router_weight, expert_ids, gate_train, up_train, down_train):
    attended = attend(queries, key_cache, value_cache, new_key, new_value, cache_lengths)
    expert_mix = mix_experts(hidden_in, norm_gain, router_weight, expert_ids, gate_train, up_train, down_train)
    return (attended, expert_mix)
```

```python
import functools
import math

import jax
import jax.numpy as jnp
from jax import lax
from jax.experimental import pallas as pl
from jax.experimental.pallas import tpu as pltpu
from jax.sharding import Mesh
from jax.sharding import PartitionSpec as P

HEADS = 32
KV_HEADS = 4
HEAD_DIM = 128
CTX = 64
EPSILON = 1e-06
SLOTS = 16
TEAM = 4
LANES = 128

MESH = pl.DeviceIdType.MESH
EXPERT = ("z", "core")
ALL = ("team", "quad", "z", "core")


def rms_normed(hidden_in, norm_gain):
    values = hidden_in.astype(jnp.float32)
    mean_square = jnp.mean(values * values, axis=-1, keepdims=True)
    return (values * lax.rsqrt(mean_square + EPSILON) * norm_gain.astype(jnp.float32)).astype(
        jnp.bfloat16
    )


def attend(queries, key_cache, value_cache, new_key, new_value, cache_lengths):
    seq_count = queries.shape[0]
    group_size = HEADS // KV_HEADS
    query_blocks = queries.reshape(seq_count, KV_HEADS, group_size, HEAD_DIM)
    cached_keys = key_cache.reshape(seq_count, CTX, KV_HEADS, HEAD_DIM)
    cached_values = value_cache.reshape(seq_count, CTX, KV_HEADS, HEAD_DIM)
    fresh_keys = new_key.reshape(seq_count, KV_HEADS, HEAD_DIM)
    fresh_values = new_value.astype(jnp.float32).reshape(seq_count, KV_HEADS, HEAD_DIM)
    score_scale = 1.0 / math.sqrt(HEAD_DIM)
    scores = (
        jnp.einsum("sgrd,scgd->sgrc", query_blocks, cached_keys, preferred_element_type=jnp.float32)
        * score_scale
    )
    own_score = (
        jnp.einsum("sgrd,sgd->sgr", query_blocks, fresh_keys, preferred_element_type=jnp.float32)
        * score_scale
    )
    positions = jnp.arange(CTX, dtype=jnp.int32)
    visible = positions[None, :] < cache_lengths[:, None]
    scores = jnp.where(visible[:, None, None, :], scores, -1e30)
    largest = jnp.maximum(jnp.max(scores, axis=-1), own_score)
    cached_exp = jnp.exp(scores - largest[..., None])
    own_exp = jnp.exp(own_score - largest)
    prob_total = jnp.sum(cached_exp, axis=-1) + own_exp
    cached_prob = (cached_exp / prob_total[..., None]).astype(jnp.bfloat16)
    own_prob = (own_exp / prob_total).astype(jnp.bfloat16).astype(jnp.float32)
    context = jnp.einsum(
        "sgrc,scgd->sgrd", cached_prob, cached_values, preferred_element_type=jnp.float32
    )
    context = context + own_prob[..., None] * fresh_values[:, :, None, :]
    return context.reshape(seq_count, HEADS * HEAD_DIM).astype(jnp.bfloat16)


def remote(src, dst, send, recv, to):
    return pltpu.make_async_remote_copy(
        src_ref=src, dst_ref=dst, send_sem=send, recv_sem=recv, device_id=to, device_id_type=MESH
    )


def wait_bytes(ref, sem):
    pltpu.make_async_copy(ref, ref, sem).wait()


def weights_kernel(nz, p_ref, out_ref, own_sem, send_sem, fwd_sem, recv_sem, mate_sem):
    quad, z, core = lax.axis_index("quad"), lax.axis_index("z"), lax.axis_index("core")
    me = z * 2 + core
    barrier = pltpu.get_barrier_semaphore()

    def greet(i, carry):
        for cc in range(2):
            pl.semaphore_signal(
                barrier, inc=1, device_id={"z": lax.rem(z + i, nz), "core": cc}, device_id_type=MESH
            )
        return carry

    lax.fori_loop(1, nz, greet, 0)
    pl.semaphore_signal(barrier, inc=1, device_id={"core": 1 - core}, device_id_type=MESH)
    for m in range(1, TEAM):
        pl.semaphore_signal(
            barrier, inc=1, device_id={"quad": lax.rem(quad + m, TEAM)}, device_id_type=MESH
        )
    pl.semaphore_wait(barrier, 2 * (nz - 1) + 1 + TEAM - 1)

    own = pltpu.make_async_copy(p_ref.at[me], out_ref.at[quad, me], own_sem)
    own.start()
    remote(
        p_ref.at[z * 2 + 1 - core], out_ref.at[quad, me], send_sem, recv_sem.at[0], {"core": 1 - core}
    ).start()

    def offset(i):
        k = i // 2 + 1
        return k + (i % 2) * (nz - 2 * k)

    def send(i, carry):
        ahead = offset(i)
        zz = lax.rem(z + ahead, nz)
        for cc in range(2):
            remote(
                p_ref.at[zz * 2 + cc],
                out_ref.at[quad, me],
                send_sem,
                recv_sem.at[ahead],
                {"z": zz, "core": cc},
            ).start()
        return carry

    lax.fori_loop(0, nz - 1, send, 0)

    def share(zz):
        rows = out_ref.at[quad, pl.ds(zz * 2, 2)]
        for m in range(1, TEAM):
            remote(
                rows, rows, fwd_sem, mate_sem.at[m - 1], {"quad": lax.rem(quad + m, TEAM)}
            ).start()

    own.wait()
    wait_bytes(out_ref.at[quad, z * 2 + 1 - core], recv_sem.at[0])
    share(z)

    def forward(i, carry):
        ahead = offset(i)
        zz = lax.rem(z - ahead + nz, nz)
        wait_bytes(out_ref.at[quad, pl.ds(zz * 2, 2)], recv_sem.at[ahead])
        share(zz)
        return carry

    lax.fori_loop(0, nz - 1, forward, 0)
    for m in range(1, TEAM):
        wait_bytes(out_ref.at[lax.rem(quad - m + TEAM, TEAM)], mate_sem.at[m - 1])
    wait_bytes(p_ref.at[pl.ds(0, 2 * nz - 1)], send_sem)
    wait_bytes(out_ref.at[pl.ds(0, TEAM - 1)], fwd_sem)


def move_weights(packed, nz):
    messages, rows, lanes = packed.shape
    return pl.pallas_call(
        functools.partial(weights_kernel, nz),
        name="move_weights",
        out_shape=jax.ShapeDtypeStruct((TEAM, messages, rows, lanes), packed.dtype),
        in_specs=[pl.BlockSpec(memory_space=pl.ANY)],
        out_specs=pl.BlockSpec(memory_space=pl.ANY),
        scratch_shapes=[
            pltpu.SemaphoreType.DMA,
            pltpu.SemaphoreType.DMA,
            pltpu.SemaphoreType.DMA,
            pltpu.SemaphoreType.DMA((nz,)),
            pltpu.SemaphoreType.DMA((TEAM - 1,)),
        ],
        compiler_params=pltpu.CompilerParams(collective_id=0, has_side_effects=True),
    )(packed)


def experts_kernel(
    nz,
    x_ref,
    meta_ref,
    w_ref,
    d_ref,
    o_ref,
    tokens,
    metas,
    wgu,
    mine,
    theirs,
    outgoing,
    acc,
    picked,
    hidden,
    sels,
    upper,
    local_sem,
    load_sem,
    ring_send,
    ring_meta_send,
    pair_send,
    pair_meta_send,
    out_send,
    sum_send,
    ring_recv,
    ring_meta,
    pair_recv,
    pair_meta,
    their_recv,
    sum_recv,
):
    half_ring = nz // 2
    z, core = lax.axis_index("z"), lax.axis_index("core")
    rows = x_ref.shape[0]
    half = rows // 2
    width = x_ref.shape[1]
    partner = {"core": 1 - core}
    after = {"z": lax.rem(z + 1, nz)}
    before = {"z": lax.rem(z + nz - 1, nz)}
    towards = (after, before)

    loads = [pltpu.make_async_copy(x_ref, tokens.at[z, 0], local_sem.at[0])]
    loads.append(pltpu.make_async_copy(meta_ref, metas.at[z, 0], local_sem.at[1]))
    for copy in loads:
        copy.start()
    strips = wgu.shape[2] // TEAM // LANES
    gate_rows = wgu.shape[1]
    weight_loads = []
    for quarter in range(TEAM):
        for strip in range(strips):
            weight_loads.append(
                pltpu.make_async_copy(
                    w_ref.at[quarter, :, pl.ds(strip * gate_rows, gate_rows), :],
                    wgu.at[:, :, pl.ds((quarter * strips + strip) * LANES, LANES)],
                    load_sem.at[quarter * strips + strip],
                )
            )
    for copy in weight_loads:
        copy.start()

    barrier = pltpu.get_barrier_semaphore()
    for who in (after, before, partner):
        pl.semaphore_signal(barrier, inc=1, device_id=who, device_id_type=MESH)
    pl.semaphore_wait(barrier, 3)
    for copy in loads:
        copy.wait()

    def chip_behind(way, s):
        return lax.rem(z + (nz - s if way == 0 else s), nz)

    def ring(way, s, part):
        at = tokens.at[chip_behind(way, s - 1), 0, pl.ds(part * half, half)]
        return remote(at, at, ring_send, ring_recv.at[way, s - 1, part], towards[way])

    def ring_metas(way, s):
        at = metas.at[chip_behind(way, s - 1), 0]
        return remote(at, at, ring_meta_send, ring_meta.at[way, s - 1], towards[way])

    def wait_ring(way, s, part):
        wait_bytes(
            tokens.at[chip_behind(way, s), 0, pl.ds(part * half, half)],
            ring_recv.at[way, s - 1, part],
        )

    def wait_ring_meta(way, s):
        wait_bytes(metas.at[chip_behind(way, s), 0], ring_meta.at[way, s - 1])

    def pair_up(t, way, s):
        remote(
            tokens.at[t, 0], tokens.at[t, 1], pair_send, pair_recv.at[way, s - 1], partner
        ).start()
        remote(
            metas.at[t, 0], metas.at[t, 1], pair_meta_send, pair_meta.at[way, s - 1], partner
        ).start()

    def wait_pair(t, way, s):
        wait_bytes(tokens.at[t, 1], pair_recv.at[way, s - 1])
        wait_bytes(metas.at[t, 1], pair_meta.at[way, s - 1])

    for way in range(2):
        ring_metas(way, 1).start()
        for part in range(2):
            ring(way, 1, part).start()
    pair_up(z, 1, half_ring)

    across = lax.broadcasted_iota(jnp.int32, (LANES, LANES), 1)
    down = lax.broadcasted_iota(jnp.int32, (LANES, LANES), 0)
    upper[...] = jnp.where(
        (down < across) & ((down >= rows) == (across >= rows)), 1.0, 0.0
    ).astype(jnp.bfloat16)
    for copy in weight_loads:
        copy.wait()

    expert = (z * 2 + core).astype(jnp.float32)

    def routing(t):
        own, other = metas[t, 0], metas[t, 1]
        lane = lax.broadcasted_iota(jnp.int32, own.shape, 1)
        ids = jnp.where(lane < rows, own, pltpu.roll(other, rows, 1))
        weights = jnp.where(lane < rows, pltpu.roll(own, rows, 1), other)
        same = ids == expert
        hit = jnp.sum(jnp.where(same, 1.0, 0.0), axis=0, keepdims=True)
        mix = jnp.sum(jnp.where(same, weights, 0.0), axis=0, keepdims=True)
        hits = jnp.broadcast_to(hit, own.shape).astype(jnp.bfloat16)
        rank = jnp.dot(hits, upper[...], preferred_element_type=jnp.float32)[0:1]
        lane = lax.broadcasted_iota(jnp.int32, (2 * SLOTS, LANES), 1)
        slot = lax.broadcasted_iota(jnp.int32, (2 * SLOTS, LANES), 0)
        rank = rank + jnp.where(lane < rows, 0.0, float(SLOTS))
        sel = jnp.where((slot.astype(jnp.float32) == rank) & (hit > 0.5), 1.0, 0.0)
        return sel, jnp.sum(sel * mix, axis=1, keepdims=True)

    def chips(s):
        return (lax.rem(z - s + nz, nz), lax.rem(z + lax.rem(s, half_ring), nz))

    def first_part(s):
        mixes = []
        for i, t in enumerate(chips(s)):
            sel, mix = routing(t)
            sels[i] = sel
            mixes.append(mix)
            picked[pl.ds(2 * SLOTS * i, 2 * SLOTS), :] = jnp.dot(
                sel.astype(jnp.bfloat16),
                tokens[t].reshape(2 * rows, width),
                preferred_element_type=jnp.float32,
            ).astype(jnp.bfloat16)
        mix = jnp.concatenate(mixes, axis=0)
        gate_up = jnp.dot(
            picked[...], wgu[...].reshape(width, -1), preferred_element_type=jnp.float32
        )
        ff = gate_up.shape[1] // 2
        gate, up = gate_up[:, :ff], gate_up[:, ff:]
        hidden[...] = (gate / (1.0 + jnp.exp(-gate)) * up * mix).astype(jnp.bfloat16)

    def second_part(s):
        spot = lax.rem(s, 2)

        @pl.when(s > 2)
        def _():
            wait_bytes(outgoing.at[spot], out_send.at[spot])

        rows_out = jnp.dot(hidden[...], d_ref[...], preferred_element_type=jnp.float32).astype(
            jnp.bfloat16
        )
        for i, t in enumerate(chips(s)):
            spread = lax.dot_general(
                sels[i].astype(jnp.bfloat16),
                rows_out[2 * SLOTS * i : 2 * SLOTS * (i + 1)],
                (((0,), (0,)), ((), ())),
                preferred_element_type=jnp.float32,
            ).astype(jnp.bfloat16)
            mine[t] = spread[:rows]
            outgoing[spot, i] = spread[rows:]
        for i, t in enumerate(chips(s)):
            remote(
                outgoing.at[spot, i],
                theirs.at[t],
                out_send.at[spot],
                their_recv.at[i, s - 1],
                partner,
            ).start()

    def wait_chunk(s):
        wait_pair(chip_behind(0, s), 0, s)
        wait_pair(chip_behind(1, s), 1, s)

    def step(s, carry):
        for way in range(2):
            wait_ring_meta(way, s)
            ring_metas(way, s + 1).start()
            wait_ring(way, s, 0)
            ring(way, s + 1, 0).start()

        @pl.when(s > 1)
        def _():
            wait_chunk(s - 1)
            first_part(s - 1)

        for way in range(2):
            wait_ring(way, s, 1)
            ring(way, s + 1, 1).start()
            pair_up(chip_behind(way, s), way, s)

        @pl.when(s > 1)
        def _():
            second_part(s - 1)

        return carry

    lax.fori_loop(1, half_ring - 1, step, 0)

    s = half_ring - 1
    for way in range(2):
        wait_ring_meta(way, s)
        if way == 0:
            ring_metas(way, s + 1).start()
        wait_ring(way, s, way)
        ring(way, s + 1, way).start()
        wait_ring(way, s, 1 - way)
        pair_up(chip_behind(way, s), way, s)
    wait_chunk(s - 1)
    first_part(s - 1)
    second_part(s - 1)

    s = half_ring
    wait_ring_meta(0, s)
    wait_ring(0, s, 0)
    wait_ring(1, s, 1)
    far = chip_behind(0, s)
    pair_up(far, 0, s)
    wait_chunk(s - 1)
    first_part(s - 1)
    second_part(s - 1)
    wait_pair(far, 0, s)
    wait_pair(z, 1, s)
    first_part(s)
    second_part(s)

    def block(way, d):
        return lax.rem(z + (d if way == 0 else nz - d), nz)

    def wait_their(i, s):
        wait_bytes(theirs.at[chips(s)[i]], their_recv.at[i, s - 1])

    def onward(way, j, part):
        return remote(
            acc.at[way, j, pl.ds(part * half, half)],
            acc.at[way, j + 1, pl.ds(part * half, half)],
            sum_send,
            sum_recv.at[way, j, part],
            towards[way],
        )

    def add(way, j, t, part, fresh):
        at = pl.ds(part * half, half)
        total = mine[t, at, :].astype(jnp.float32) + theirs[t, at, :].astype(jnp.float32)
        if not fresh:
            total = total + acc[way, j, at, :].astype(jnp.float32)
        acc[way, j, at, :] = total.astype(jnp.bfloat16)

    def wait_sum(way, j, part):
        wait_bytes(acc.at[way, j, pl.ds(part * half, half)], sum_recv.at[way, j - 1, part])

    wait_their(0, half_ring)
    for way in range(2):
        add(way, 0, far, way, True)
    for way in range(2):
        onward(way, 0, way).start()

    d = half_ring - 1
    wait_their(0, d)
    wait_their(1, d)
    for way in range(2):
        add(way, 1, block(way, d), 1 - way, True)
    for way in range(2):
        onward(way, 1, 1 - way).start()
    for way in range(2):
        wait_sum(way, 1, way)
        add(way, 1, block(way, d), way, False)
    for way in range(2):
        onward(way, 1, way).start()

    def sums(j, carry):
        d = half_ring - j
        wait_their(0, d)
        wait_their(1, d)
        for part in range(2):
            for way in range(2):
                wait_sum(way, j, part)
                add(way, j, block(way, d), part, False)
            for way in range(2):
                onward(way, j, part).start()
        return carry

    lax.fori_loop(2, half_ring, sums, 0)

    wait_their(1, half_ring)
    for part in range(2):
        at = pl.ds(part * half, half)
        for way in range(2):
            wait_sum(way, half_ring, part)
        o_ref[at, :] = (
            mine[z, at, :].astype(jnp.float32)
            + theirs[z, at, :].astype(jnp.float32)
            + acc[0, half_ring, at, :].astype(jnp.float32)
            + acc[1, half_ring, at, :].astype(jnp.float32)
        ).astype(jnp.bfloat16)

    wait_bytes(mine.at[pl.ds(0, nz - 1)], ring_send)
    wait_bytes(metas.at[pl.ds(0, nz - 1), 0], ring_meta_send)
    wait_bytes(mine, pair_send)
    wait_bytes(metas.at[:, 0], pair_meta_send)
    wait_bytes(mine.at[pl.ds(0, nz - 1)], sum_send)
    wait_bytes(outgoing.at[0], out_send.at[0])
    wait_bytes(outgoing.at[1], out_send.at[1])


def experts(normed, meta, moved, down, nz):
    rows, width = normed.shape
    ff = down.shape[0]
    bf16 = jnp.bfloat16
    steps = nz // 2
    dma = pltpu.SemaphoreType.DMA
    return pl.pallas_call(
        functools.partial(experts_kernel, nz),
        name="experts",
        out_shape=jax.ShapeDtypeStruct((rows, width), bf16),
        in_specs=[
            pl.BlockSpec(memory_space=pl.ANY),
            pl.BlockSpec(memory_space=pl.ANY),
            pl.BlockSpec(memory_space=pl.ANY),
            pl.BlockSpec(memory_space=pltpu.VMEM),
        ],
        out_specs=pl.BlockSpec(memory_space=pltpu.VMEM),
        scratch_shapes=[
            pltpu.VMEM((nz, 2, rows, width), bf16),
            pltpu.VMEM((nz, 2, 8, LANES), jnp.float32),
            pltpu.VMEM((2 * nz, width // (2 * nz), 2 * ff), bf16),
            pltpu.VMEM((nz, rows, width), bf16),
            pltpu.VMEM((nz, rows, width), bf16),
            pltpu.VMEM((2, 2, rows, width), bf16),
            pltpu.VMEM((2, steps + 1, rows, width), bf16),
            pltpu.VMEM((4 * SLOTS, width), bf16),
            pltpu.VMEM((4 * SLOTS, ff), bf16),
            pltpu.VMEM((2, 2 * SLOTS, LANES), jnp.float32),
            pltpu.VMEM((LANES, LANES), bf16),
            dma((2,)),
            dma((3 * TEAM,)),
            dma,
            dma,
            dma,
            dma,
            dma((2,)),
            dma,
            dma((2, steps, 2)),
            dma((2, steps)),
            dma((2, steps)),
            dma((2, steps)),
            dma((2, steps)),
            dma((2, steps, 2)),
        ],
        compiler_params=pltpu.CompilerParams(
            collective_id=1, has_side_effects=True, vmem_limit_bytes=60 << 20
        ),
    )(normed, meta, moved, down)


def pack(gate, up, down, quad):
    count, gate_rows, ff = gate.shape
    down_rows, width = down.shape[1:]
    cut, down_cut = 2 * ff // TEAM, width // TEAM
    start = lax.rem(quad, TEAM // 2) * cut
    gate_up = jnp.where(
        quad < TEAM // 2,
        lax.dynamic_slice_in_dim(gate, start, cut, 2),
        lax.dynamic_slice_in_dim(up, start, cut, 2),
    )
    down = lax.dynamic_slice_in_dim(down, quad * down_cut, down_cut, 2)
    strips = [
        jnp.swapaxes(a.reshape(count, a.shape[1], -1, LANES), 1, 2).reshape(count, -1, LANES)
        for a in (gate_up, down)
    ]
    return jnp.concatenate(strips, axis=1)


def local(
    nz,
    queries,
    key_cache,
    value_cache,
    new_key,
    new_value,
    cache_lengths,
    hidden_in,
    norm_gain,
    router_weight,
    expert_ids,
    gate_train,
    up_train,
    down_train,
):
    quad = lax.axis_index("quad")
    moved = move_weights(pack(gate_train, up_train, down_train, quad), nz)
    attended = attend(queries, key_cache, value_cache, new_key, new_value, cache_lengths)

    normed = rms_normed(hidden_in, norm_gain)
    logits = jnp.dot(normed, router_weight, preferred_element_type=jnp.float32)
    expert_range = jnp.arange(router_weight.shape[1], dtype=jnp.int32)
    picked = expert_ids[:, :, None] == expert_range[None, None, :]
    chosen = jnp.sum(jnp.where(picked, logits[:, None, :], 0.0), axis=-1)
    mixing = jax.nn.softmax(chosen, axis=-1)
    meta = jnp.concatenate([expert_ids.astype(jnp.float32).T, mixing.T], axis=1)

    gate_rows, down_rows = gate_train.shape[1], down_train.shape[1]
    strips = 2 * gate_train.shape[2] // TEAM // LANES
    down = moved[:, :, strips * gate_rows :, :].reshape(TEAM, 2 * nz, -1, down_rows, LANES)
    down = jnp.transpose(down, (1, 3, 0, 2, 4)).reshape(2 * nz * down_rows, -1)
    return attended, experts(normed, meta, moved, down, nz)


def solution(mesh):
    groups, nz = mesh.shape["groups"], mesh.shape["expert"] // 2
    torus = Mesh(mesh.devices.reshape(groups // TEAM, TEAM, nz, 2), ALL)
    placed = (
        P(ALL, None),
        P(ALL, None, None),
        P(ALL, None, None),
        P(ALL, None),
        P(ALL, None),
        P(ALL),
        P(ALL, None),
        P(),
        P(),
        P(ALL, None),
        P(None, EXPERT, None),
        P(None, EXPERT, None),
        P(None, EXPERT, None),
    )
    return jax.shard_map(
        functools.partial(local, nz),
        mesh=torus,
        in_specs=placed,
        out_specs=(P(ALL, None), P(ALL, None)),
        check_vma=False,
    )
```

```python
import functools
import math

import jax
import jax.numpy as jnp
from jax import lax
from jax.experimental import pallas as pl
from jax.experimental.pallas import tpu as pltpu
from jax.sharding import Mesh
from jax.sharding import PartitionSpec as P

HEADS = 32
KV_HEADS = 4
HEAD_DIM = 128
CTX = 64
EPSILON = 1e-06
SLOTS = 16
TEAM = 4
LANES = 128

MESH = pl.DeviceIdType.MESH
EXPERT = ("z", "core")
ALL = ("team", "quad", "z", "core")


def rms_normed(hidden_in, norm_gain):
    values = hidden_in.astype(jnp.float32)
    mean_square = jnp.mean(values * values, axis=-1, keepdims=True)
    return (values * lax.rsqrt(mean_square + EPSILON) * norm_gain.astype(jnp.float32)).astype(
        jnp.bfloat16
    )


def attend(queries, key_cache, value_cache, new_key, new_value, cache_lengths):
    seq_count = queries.shape[0]
    group_size = HEADS // KV_HEADS
    query_blocks = queries.reshape(seq_count, KV_HEADS, group_size, HEAD_DIM)
    cached_keys = key_cache.reshape(seq_count, CTX, KV_HEADS, HEAD_DIM)
    cached_values = value_cache.reshape(seq_count, CTX, KV_HEADS, HEAD_DIM)
    fresh_keys = new_key.reshape(seq_count, KV_HEADS, HEAD_DIM)
    fresh_values = new_value.astype(jnp.float32).reshape(seq_count, KV_HEADS, HEAD_DIM)
    score_scale = 1.0 / math.sqrt(HEAD_DIM)
    scores = (
        jnp.einsum("sgrd,scgd->sgrc", query_blocks, cached_keys, preferred_element_type=jnp.float32)
        * score_scale
    )
    own_score = (
        jnp.einsum("sgrd,sgd->sgr", query_blocks, fresh_keys, preferred_element_type=jnp.float32)
        * score_scale
    )
    positions = jnp.arange(CTX, dtype=jnp.int32)
    visible = positions[None, :] < cache_lengths[:, None]
    scores = jnp.where(visible[:, None, None, :], scores, -1e30)
    largest = jnp.maximum(jnp.max(scores, axis=-1), own_score)
    cached_exp = jnp.exp(scores - largest[..., None])
    own_exp = jnp.exp(own_score - largest)
    prob_total = jnp.sum(cached_exp, axis=-1) + own_exp
    cached_prob = (cached_exp / prob_total[..., None]).astype(jnp.bfloat16)
    own_prob = (own_exp / prob_total).astype(jnp.bfloat16).astype(jnp.float32)
    context = jnp.einsum(
        "sgrc,scgd->sgrd", cached_prob, cached_values, preferred_element_type=jnp.float32
    )
    context = context + own_prob[..., None] * fresh_values[:, :, None, :]
    return context.reshape(seq_count, HEADS * HEAD_DIM).astype(jnp.bfloat16)


def remote(src, dst, send, recv, to):
    return pltpu.make_async_remote_copy(
        src_ref=src, dst_ref=dst, send_sem=send, recv_sem=recv, device_id=to, device_id_type=MESH
    )


def wait_bytes(ref, sem):
    pltpu.make_async_copy(ref, ref, sem).wait()


def weights_kernel(
    nz, p_ref, out_ref, transit, own_sem, pair_send, ring_send, fwd_sem, recv_sem, hop_recv, mate_sem
):
    quad, z, core = lax.axis_index("quad"), lax.axis_index("z"), lax.axis_index("core")
    half_ring = nz // 2
    me = z * 2 + core
    partner = {"core": 1 - core}

    def chip(way, steps):
        return lax.rem(z + (steps if way == 0 else nz - steps), nz)

    next_chip = (chip(0, 1), chip(1, 1))
    barrier = pltpu.get_barrier_semaphore()
    friends = [{"z": next_chip[way], "core": cc} for way in range(2) for cc in range(2)]
    friends += [partner] + [{"quad": lax.rem(quad + m, TEAM)} for m in range(1, TEAM)]
    for who in friends:
        pl.semaphore_signal(barrier, inc=1, device_id=who, device_id_type=MESH)
    pl.semaphore_wait(barrier, len(friends))

    own = pltpu.make_async_copy(p_ref.at[me], out_ref.at[quad, me], own_sem)
    own.start()

    def place(hops, dist):
        return half_ring * (hops - 1) - hops * (hops - 1) // 2 + half_ring - dist

    def pair_at(hops, way, dist):
        return transit.at[way, place(hops, dist)]

    def single_at(hops, way):
        return transit.at[way, place(hops, half_ring), pl.ds(0, 1)]

    def pass_on(way, src, dst, hops, dist):
        remote(
            src, dst, ring_send.at[way], hop_recv.at[way, place(hops, dist)], {"z": next_chip[way]}
        ).start()

    def deliver(way, src, hops, dist, cc):
        remote(
            src,
            out_ref.at[quad, chip(way, nz - hops) * 2 + core],
            ring_send.at[way],
            recv_sem.at[dist if way == 0 else nz - dist],
            {"z": next_chip[way], "core": cc},
        ).start()

    def share(zz):
        rows = out_ref.at[quad, pl.ds(zz * 2, 2)]
        for m in range(1, TEAM):
            remote(
                rows, rows, fwd_sem, mate_sem.at[m - 1], {"quad": lax.rem(quad + m, TEAM)}
            ).start()

    def arrived(ahead):
        zz = lax.rem(z - ahead + nz, nz)
        wait_bytes(out_ref.at[quad, pl.ds(zz * 2, 2)], recv_sem.at[ahead])
        share(zz)

    for way in range(2):
        at = pl.ds(chip(way, half_ring) * 2 + way, 1)
        pass_on(way, p_ref.at[at], single_at(1, way), 1, half_ring)

    def first(i, carry):
        dist = half_ring - 1 - i
        for way in range(2):
            at = pl.ds(chip(way, dist) * 2, 2)
            pass_on(way, p_ref.at[at], pair_at(1, way, dist), 1, dist)
        return carry

    lax.fori_loop(0, half_ring - 2, first, 0)
    for way in range(2):
        for cc in range(2):
            deliver(way, p_ref.at[chip(way, 1) * 2 + cc], 0, 1, cc)
    remote(
        p_ref.at[z * 2 + 1 - core], out_ref.at[quad, me], pair_send, recv_sem.at[0], partner
    ).start()
    own.wait()
    wait_bytes(out_ref.at[quad, z * 2 + 1 - core], recv_sem.at[0])
    share(z)

    def relay(hops, carry):
        for way in range(2):
            src = single_at(hops, way)
            wait_bytes(src, hop_recv.at[way, place(hops, half_ring)])
            pass_on(way, src, single_at(hops + 1, way), hops + 1, half_ring)

        def through(i, carry):
            dist = half_ring - 1 - i
            for way in range(2):
                src = pair_at(hops, way, dist)
                wait_bytes(src, hop_recv.at[way, place(hops, dist)])
                pass_on(way, src, pair_at(hops + 1, way, dist), hops + 1, dist)
            return carry

        lax.fori_loop(0, half_ring - 2 - hops, through, 0)
        for way in range(2):
            src = pair_at(hops, way, hops + 1)
            wait_bytes(src, hop_recv.at[way, place(hops, hops + 1)])
            for cc in range(2):
                deliver(way, src.at[cc], hops, hops + 1, cc)
        arrived(hops)
        arrived(nz - hops)
        return carry

    lax.fori_loop(1, half_ring - 1, relay, 0)
    hops = half_ring - 1
    for way in range(2):
        src = single_at(hops, way)
        wait_bytes(src, hop_recv.at[way, place(hops, half_ring)])
        deliver(way, src.at[0], hops, half_ring, way)
    arrived(hops)
    arrived(nz - hops)
    arrived(half_ring)
    for m in range(1, TEAM):
        wait_bytes(out_ref.at[lax.rem(quad - m + TEAM, TEAM)], mate_sem.at[m - 1])
    wait_bytes(p_ref.at[0], pair_send)
    for way in range(2):
        wait_bytes(out_ref.at[pl.ds(0, nz // 8)], ring_send.at[way])
    wait_bytes(out_ref.at[pl.ds(0, TEAM - 1)], fwd_sem)


def move_weights(packed, nz):
    messages, rows, lanes = packed.shape
    half_ring = nz // 2
    places = half_ring * (half_ring - 1) // 2
    dma = pltpu.SemaphoreType.DMA
    return pl.pallas_call(
        functools.partial(weights_kernel, nz),
        name="move_weights",
        out_shape=(
            jax.ShapeDtypeStruct((TEAM, messages, rows, lanes), packed.dtype),
            jax.ShapeDtypeStruct((2, places, 2, rows, lanes), packed.dtype),
        ),
        in_specs=[pl.BlockSpec(memory_space=pl.ANY)],
        out_specs=[pl.BlockSpec(memory_space=pl.ANY)] * 2,
        scratch_shapes=[
            dma,
            dma,
            dma((2,)),
            dma,
            dma((nz,)),
            dma((2, places)),
            dma((TEAM - 1,)),
        ],
        compiler_params=pltpu.CompilerParams(collective_id=0, has_side_effects=True),
    )(packed)[0]


def experts_kernel(
    nz,
    x_ref,
    meta_ref,
    w_ref,
    d_ref,
    o_ref,
    tokens,
    metas,
    wgu,
    mine,
    theirs,
    outgoing,
    acc,
    picked,
    hidden,
    sels,
    upper,
    local_sem,
    load_sem,
    ring_send,
    ring_meta_send,
    pair_send,
    pair_meta_send,
    out_send,
    sum_send,
    ring_recv,
    ring_meta,
    pair_recv,
    pair_meta,
    their_recv,
    sum_recv,
):
    half_ring = nz // 2
    z, core = lax.axis_index("z"), lax.axis_index("core")
    rows = x_ref.shape[0]
    half = rows // 2
    width = x_ref.shape[1]
    partner = {"core": 1 - core}
    after = {"z": lax.rem(z + 1, nz)}
    before = {"z": lax.rem(z + nz - 1, nz)}
    towards = (after, before)

    loads = [pltpu.make_async_copy(x_ref, tokens.at[z, 0], local_sem.at[0])]
    loads.append(pltpu.make_async_copy(meta_ref, metas.at[z, 0], local_sem.at[1]))
    for copy in loads:
        copy.start()
    strips = wgu.shape[2] // TEAM // LANES
    gate_rows = wgu.shape[1]
    weight_loads = []
    for quarter in range(TEAM):
        for strip in range(strips):
            weight_loads.append(
                pltpu.make_async_copy(
                    w_ref.at[quarter, :, pl.ds(strip * gate_rows, gate_rows), :],
                    wgu.at[:, :, pl.ds((quarter * strips + strip) * LANES, LANES)],
                    load_sem.at[quarter * strips + strip],
                )
            )
    for copy in weight_loads:
        copy.start()

    barrier = pltpu.get_barrier_semaphore()
    for who in (after, before, partner):
        pl.semaphore_signal(barrier, inc=1, device_id=who, device_id_type=MESH)
    pl.semaphore_wait(barrier, 3)
    for copy in loads:
        copy.wait()

    def chip_behind(way, s):
        return lax.rem(z + (nz - s if way == 0 else s), nz)

    def ring(way, s, part):
        at = tokens.at[chip_behind(way, s - 1), 0, pl.ds(part * half, half)]
        return remote(at, at, ring_send, ring_recv.at[way, s - 1, part], towards[way])

    def ring_metas(way, s):
        at = metas.at[chip_behind(way, s - 1), 0]
        return remote(at, at, ring_meta_send, ring_meta.at[way, s - 1], towards[way])

    def wait_ring(way, s, part):
        wait_bytes(
            tokens.at[chip_behind(way, s), 0, pl.ds(part * half, half)],
            ring_recv.at[way, s - 1, part],
        )

    def wait_ring_meta(way, s):
        wait_bytes(metas.at[chip_behind(way, s), 0], ring_meta.at[way, s - 1])

    def pair_up(t, way, s):
        remote(
            tokens.at[t, 0], tokens.at[t, 1], pair_send, pair_recv.at[way, s - 1], partner
        ).start()
        remote(
            metas.at[t, 0], metas.at[t, 1], pair_meta_send, pair_meta.at[way, s - 1], partner
        ).start()

    def wait_pair(t, way, s):
        wait_bytes(tokens.at[t, 1], pair_recv.at[way, s - 1])
        wait_bytes(metas.at[t, 1], pair_meta.at[way, s - 1])

    for way in range(2):
        ring_metas(way, 1).start()
        for part in range(2):
            ring(way, 1, part).start()
    pair_up(z, 1, half_ring)

    across = lax.broadcasted_iota(jnp.int32, (LANES, LANES), 1)
    down = lax.broadcasted_iota(jnp.int32, (LANES, LANES), 0)
    upper[...] = jnp.where(
        (down < across) & ((down >= rows) == (across >= rows)), 1.0, 0.0
    ).astype(jnp.bfloat16)
    for copy in weight_loads:
        copy.wait()

    expert = (z * 2 + core).astype(jnp.float32)

    def routing(t):
        own, other = metas[t, 0], metas[t, 1]
        lane = lax.broadcasted_iota(jnp.int32, own.shape, 1)
        ids = jnp.where(lane < rows, own, pltpu.roll(other, rows, 1))
        weights = jnp.where(lane < rows, pltpu.roll(own, rows, 1), other)
        same = ids == expert
        hit = jnp.sum(jnp.where(same, 1.0, 0.0), axis=0, keepdims=True)
        mix = jnp.sum(jnp.where(same, weights, 0.0), axis=0, keepdims=True)
        hits = jnp.broadcast_to(hit, own.shape).astype(jnp.bfloat16)
        rank = jnp.dot(hits, upper[...], preferred_element_type=jnp.float32)[0:1]
        lane = lax.broadcasted_iota(jnp.int32, (2 * SLOTS, LANES), 1)
        slot = lax.broadcasted_iota(jnp.int32, (2 * SLOTS, LANES), 0)
        rank = rank + jnp.where(lane < rows, 0.0, float(SLOTS))
        sel = jnp.where((slot.astype(jnp.float32) == rank) & (hit > 0.5), 1.0, 0.0)
        return sel, jnp.sum(sel * mix, axis=1, keepdims=True)

    def chips(s):
        return (lax.rem(z - s + nz, nz), lax.rem(z + lax.rem(s, half_ring), nz))

    def first_part(s):
        mixes = []
        for i, t in enumerate(chips(s)):
            sel, mix = routing(t)
            sels[i] = sel
            mixes.append(mix)
            picked[pl.ds(2 * SLOTS * i, 2 * SLOTS), :] = jnp.dot(
                sel.astype(jnp.bfloat16),
                tokens[t].reshape(2 * rows, width),
                preferred_element_type=jnp.float32,
            ).astype(jnp.bfloat16)
        mix = jnp.concatenate(mixes, axis=0)
        gate_up = jnp.dot(
            picked[...], wgu[...].reshape(width, -1), preferred_element_type=jnp.float32
        )
        ff = gate_up.shape[1] // 2
        gate, up = gate_up[:, :ff], gate_up[:, ff:]
        hidden[...] = (gate / (1.0 + jnp.exp(-gate)) * up * mix).astype(jnp.bfloat16)

    def second_part(s):
        spot = lax.rem(s, 2)

        @pl.when(s > 2)
        def _():
            wait_bytes(outgoing.at[spot], out_send.at[spot])

        rows_out = jnp.dot(hidden[...], d_ref[...], preferred_element_type=jnp.float32).astype(
            jnp.bfloat16
        )
        for i, t in enumerate(chips(s)):
            spread = lax.dot_general(
                sels[i].astype(jnp.bfloat16),
                rows_out[2 * SLOTS * i : 2 * SLOTS * (i + 1)],
                (((0,), (0,)), ((), ())),
                preferred_element_type=jnp.float32,
            ).astype(jnp.bfloat16)
            mine[t] = spread[:rows]
            outgoing[spot, i] = spread[rows:]
        for i, t in enumerate(chips(s)):
            remote(
                outgoing.at[spot, i],
                theirs.at[t],
                out_send.at[spot],
                their_recv.at[i, s - 1],
                partner,
            ).start()

    def wait_chunk(s):
        wait_pair(chip_behind(0, s), 0, s)
        wait_pair(chip_behind(1, s), 1, s)

    def step(s, carry):
        for way in range(2):
            wait_ring_meta(way, s)
            ring_metas(way, s + 1).start()
            wait_ring(way, s, 0)
            ring(way, s + 1, 0).start()

        @pl.when(s > 1)
        def _():
            wait_chunk(s - 1)
            first_part(s - 1)

        for way in range(2):
            wait_ring(way, s, 1)
            ring(way, s + 1, 1).start()
            pair_up(chip_behind(way, s), way, s)

        @pl.when(s > 1)
        def _():
            second_part(s - 1)

        return carry

    lax.fori_loop(1, half_ring - 1, step, 0)

    s = half_ring - 1
    for way in range(2):
        wait_ring_meta(way, s)
        if way == 0:
            ring_metas(way, s + 1).start()
        wait_ring(way, s, way)
        ring(way, s + 1, way).start()
        wait_ring(way, s, 1 - way)
        pair_up(chip_behind(way, s), way, s)
    wait_chunk(s - 1)
    first_part(s - 1)
    second_part(s - 1)

    s = half_ring
    wait_ring_meta(0, s)
    wait_ring(0, s, 0)
    wait_ring(1, s, 1)
    far = chip_behind(0, s)
    pair_up(far, 0, s)
    wait_chunk(s - 1)
    first_part(s - 1)
    second_part(s - 1)
    wait_pair(far, 0, s)
    wait_pair(z, 1, s)
    first_part(s)
    second_part(s)

    def block(way, d):
        return lax.rem(z + (d if way == 0 else nz - d), nz)

    def wait_their(i, s):
        wait_bytes(theirs.at[chips(s)[i]], their_recv.at[i, s - 1])

    def onward(way, j, part):
        return remote(
            acc.at[way, j, pl.ds(part * half, half)],
            acc.at[way, j + 1, pl.ds(part * half, half)],
            sum_send,
            sum_recv.at[way, j, part],
            towards[way],
        )

    def add(way, j, t, part, fresh):
        at = pl.ds(part * half, half)
        total = mine[t, at, :].astype(jnp.float32) + theirs[t, at, :].astype(jnp.float32)
        if not fresh:
            total = total + acc[way, j, at, :].astype(jnp.float32)
        acc[way, j, at, :] = total.astype(jnp.bfloat16)

    def wait_sum(way, j, part):
        wait_bytes(acc.at[way, j, pl.ds(part * half, half)], sum_recv.at[way, j - 1, part])

    wait_their(0, half_ring)
    for way in range(2):
        add(way, 0, far, way, True)
    for way in range(2):
        onward(way, 0, way).start()

    d = half_ring - 1
    wait_their(0, d)
    wait_their(1, d)
    for way in range(2):
        add(way, 1, block(way, d), 1 - way, True)
    for way in range(2):
        onward(way, 1, 1 - way).start()
    for way in range(2):
        wait_sum(way, 1, way)
        add(way, 1, block(way, d), way, False)
    for way in range(2):
        onward(way, 1, way).start()

    def sums(j, carry):
        d = half_ring - j
        wait_their(0, d)
        wait_their(1, d)
        for part in range(2):
            for way in range(2):
                wait_sum(way, j, part)
                add(way, j, block(way, d), part, False)
            for way in range(2):
                onward(way, j, part).start()
        return carry

    lax.fori_loop(2, half_ring, sums, 0)

    wait_their(1, half_ring)
    for part in range(2):
        at = pl.ds(part * half, half)
        for way in range(2):
            wait_sum(way, half_ring, part)
        o_ref[at, :] = (
            mine[z, at, :].astype(jnp.float32)
            + theirs[z, at, :].astype(jnp.float32)
            + acc[0, half_ring, at, :].astype(jnp.float32)
            + acc[1, half_ring, at, :].astype(jnp.float32)
        ).astype(jnp.bfloat16)

    wait_bytes(mine.at[pl.ds(0, nz - 1)], ring_send)
    wait_bytes(metas.at[pl.ds(0, nz - 1), 0], ring_meta_send)
    wait_bytes(mine, pair_send)
    wait_bytes(metas.at[:, 0], pair_meta_send)
    wait_bytes(mine.at[pl.ds(0, nz - 1)], sum_send)
    wait_bytes(outgoing.at[0], out_send.at[0])
    wait_bytes(outgoing.at[1], out_send.at[1])


def experts(normed, meta, moved, down, nz):
    rows, width = normed.shape
    ff = down.shape[0]
    bf16 = jnp.bfloat16
    steps = nz // 2
    dma = pltpu.SemaphoreType.DMA
    return pl.pallas_call(
        functools.partial(experts_kernel, nz),
        name="experts",
        out_shape=jax.ShapeDtypeStruct((rows, width), bf16),
        in_specs=[
            pl.BlockSpec(memory_space=pl.ANY),
            pl.BlockSpec(memory_space=pl.ANY),
            pl.BlockSpec(memory_space=pl.ANY),
            pl.BlockSpec(memory_space=pltpu.VMEM),
        ],
        out_specs=pl.BlockSpec(memory_space=pltpu.VMEM),
        scratch_shapes=[
            pltpu.VMEM((nz, 2, rows, width), bf16),
            pltpu.VMEM((nz, 2, 8, LANES), jnp.float32),
            pltpu.VMEM((2 * nz, width // (2 * nz), 2 * ff), bf16),
            pltpu.VMEM((nz, rows, width), bf16),
            pltpu.VMEM((nz, rows, width), bf16),
            pltpu.VMEM((2, 2, rows, width), bf16),
            pltpu.VMEM((2, steps + 1, rows, width), bf16),
            pltpu.VMEM((4 * SLOTS, width), bf16),
            pltpu.VMEM((4 * SLOTS, ff), bf16),
            pltpu.VMEM((2, 2 * SLOTS, LANES), jnp.float32),
            pltpu.VMEM((LANES, LANES), bf16),
            dma((2,)),
            dma((3 * TEAM,)),
            dma,
            dma,
            dma,
            dma,
            dma((2,)),
            dma,
            dma((2, steps, 2)),
            dma((2, steps)),
            dma((2, steps)),
            dma((2, steps)),
            dma((2, steps)),
            dma((2, steps, 2)),
        ],
        compiler_params=pltpu.CompilerParams(
            collective_id=1, has_side_effects=True, vmem_limit_bytes=60 << 20
        ),
    )(normed, meta, moved, down)


def pack(gate, up, down, quad):
    count, gate_rows, ff = gate.shape
    down_rows, width = down.shape[1:]
    cut, down_cut = 2 * ff // TEAM, width // TEAM
    start = lax.rem(quad, TEAM // 2) * cut
    gate_up = jnp.where(
        quad < TEAM // 2,
        lax.dynamic_slice_in_dim(gate, start, cut, 2),
        lax.dynamic_slice_in_dim(up, start, cut, 2),
    )
    down = lax.dynamic_slice_in_dim(down, quad * down_cut, down_cut, 2)
    strips = [
        jnp.swapaxes(a.reshape(count, a.shape[1], -1, LANES), 1, 2).reshape(count, -1, LANES)
        for a in (gate_up, down)
    ]
    return jnp.concatenate(strips, axis=1)


def local(
    nz,
    queries,
    key_cache,
    value_cache,
    new_key,
    new_value,
    cache_lengths,
    hidden_in,
    norm_gain,
    router_weight,
    expert_ids,
    gate_train,
    up_train,
    down_train,
):
    quad = lax.axis_index("quad")
    moved = move_weights(pack(gate_train, up_train, down_train, quad), nz)
    attended = attend(queries, key_cache, value_cache, new_key, new_value, cache_lengths)

    normed = rms_normed(hidden_in, norm_gain)
    logits = jnp.dot(normed, router_weight, preferred_element_type=jnp.float32)
    expert_range = jnp.arange(router_weight.shape[1], dtype=jnp.int32)
    picked = expert_ids[:, :, None] == expert_range[None, None, :]
    chosen = jnp.sum(jnp.where(picked, logits[:, None, :], 0.0), axis=-1)
    mixing = jax.nn.softmax(chosen, axis=-1)
    meta = jnp.concatenate([expert_ids.astype(jnp.float32).T, mixing.T], axis=1)

    gate_rows, down_rows = gate_train.shape[1], down_train.shape[1]
    strips = 2 * gate_train.shape[2] // TEAM // LANES
    down = moved[:, :, strips * gate_rows :, :].reshape(TEAM, 2 * nz, -1, down_rows, LANES)
    down = jnp.transpose(down, (1, 3, 0, 2, 4)).reshape(2 * nz * down_rows, -1)
    return attended, experts(normed, meta, moved, down, nz)


def solution(mesh):
    groups, nz = mesh.shape["groups"], mesh.shape["expert"] // 2
    torus = Mesh(mesh.devices.reshape(groups // TEAM, TEAM, nz, 2), ALL)
    placed = (
        P(ALL, None),
        P(ALL, None, None),
        P(ALL, None, None),
        P(ALL, None),
        P(ALL, None),
        P(ALL),
        P(ALL, None),
        P(),
        P(),
        P(ALL, None),
        P(None, EXPERT, None),
        P(None, EXPERT, None),
        P(None, EXPERT, None),
    )
    return jax.shard_map(
        functools.partial(local, nz),
        mesh=torus,
        in_specs=placed,
        out_specs=(P(ALL, None), P(ALL, None)),
        check_vma=False,
    )
```

```python
import functools
import math

import jax
import jax.numpy as jnp
from jax import lax
from jax.experimental import pallas as pl
from jax.experimental.pallas import tpu as pltpu
from jax.sharding import Mesh
from jax.sharding import PartitionSpec as P

HEADS = 32
KV_HEADS = 4
HEAD_DIM = 128
CTX = 64
EPSILON = 1e-06
SLOTS = 16
TEAM = 4
LANES = 128
BLOCK = 16
GU_LATE = 4
DOWN_WAIT = 3
GU_WAIT = 7

MESH = pl.DeviceIdType.MESH
EXPERT = ("z", "core")
ALL = ("team", "quad", "z", "core")


def rms_normed(hidden_in, norm_gain):
    values = hidden_in.astype(jnp.float32)
    mean_square = jnp.mean(values * values, axis=-1, keepdims=True)
    return (values * lax.rsqrt(mean_square + EPSILON) * norm_gain.astype(jnp.float32)).astype(
        jnp.bfloat16
    )


def remote(src, dst, send, recv, to):
    return pltpu.make_async_remote_copy(
        src_ref=src, dst_ref=dst, send_sem=send, recv_sem=recv, device_id=to, device_id_type=MESH
    )


def wait_bytes(ref, sem):
    pltpu.make_async_copy(ref, ref, sem).wait()


def moe_kernel(
    nz,
    x_ref,
    gain_ref,
    router_ref,
    ids_ref,
    q_ref,
    key_ref,
    value_ref,
    new_key_ref,
    new_value_ref,
    lengths_ref,
    gate_ref,
    up_ref,
    down_ref,
    o_ref,
    attended_ref,
    tokens,
    metas,
    wgu,
    down_in,
    dmat,
    gu_stage,
    down_raw,
    down_out,
    mine,
    theirs,
    outgoing,
    acc,
    picked,
    hidden,
    sels,
    upper,
    perm,
    square,
    ids_row,
    load_sem,
    raw_sem,
    own_sem,
    gu_send,
    down_send,
    gu_fwd,
    down_fwd,
    gu_recv,
    down_recv,
    gu_mate,
    down_mate,
    ring_send,
    ring_meta_send,
    pair_send,
    pair_meta_send,
    out_send,
    sum_send,
    ring_recv,
    ring_meta,
    pair_recv,
    pair_meta,
    their_recv,
    sum_recv,
):
    half_ring = nz // 2
    quad, z, core = lax.axis_index("quad"), lax.axis_index("z"), lax.axis_index("core")
    me = z * 2 + core
    rows, width = x_ref.shape
    half = rows // 2
    partner = {"core": 1 - core}
    after = {"z": lax.rem(z + 1, nz)}
    before = {"z": lax.rem(z + nz - 1, nz)}
    towards = (after, before)
    mates = [{"quad": lax.rem(quad + m, TEAM)} for m in range(1, TEAM)]
    cut = gu_stage.shape[2]
    columns = pl.ds(pl.multiple_of(quad * cut, LANES), cut)
    down_cut = width // TEAM
    down_rows = down_ref.shape[0]
    message = down_in.shape[2]
    strips = message // down_rows
    block = down_raw.shape[2]
    blocks = 2 * nz // block

    stage_from = pl.ds(pl.multiple_of(lax.rem(quad, TEAM // 2) * cut, LANES), cut)

    @pl.when(quad < TEAM // 2)
    def _():
        pltpu.make_async_copy(gate_ref.at[:, :, stage_from], gu_stage, load_sem).start()

    @pl.when(quad >= TEAM // 2)
    def _():
        pltpu.make_async_copy(up_ref.at[:, :, stage_from], gu_stage, load_sem).start()

    raw = []
    for c in range(strips):
        for g in range(blocks):
            at = pl.ds(pl.multiple_of(quad * down_cut + c * LANES, LANES), LANES)
            raw.append(
                pltpu.make_async_copy(
                    down_ref.at[:, pl.ds(g * block, block), at],
                    down_raw.at[c, :, :, pl.ds(g * LANES, LANES)],
                    raw_sem.at[c * blocks + g],
                )
            )
    for copy in raw:
        copy.start()

    barrier = pltpu.get_barrier_semaphore()

    def greet(i, carry):
        for cc in range(2):
            pl.semaphore_signal(
                barrier, inc=1, device_id={"z": lax.rem(z + i, nz), "core": cc}, device_id_type=MESH
            )
        return carry

    lax.fori_loop(1, nz, greet, 0)
    for who in [partner] + mates:
        pl.semaphore_signal(barrier, inc=1, device_id=who, device_id_type=MESH)

    across = lax.broadcasted_iota(jnp.int32, (LANES, LANES), 1)
    below = lax.broadcasted_iota(jnp.int32, (LANES, LANES), 0)
    normed = rms_normed(x_ref[...], gain_ref[...])
    tokens[z, 0] = normed
    square[...] = jnp.zeros_like(square)
    square[pl.ds(0, 2 * nz), pl.ds(0, rows)] = lax.dot_general(
        router_ref[...], normed, (((1,), (1,)), ((), ())), preferred_element_type=jnp.float32
    )
    logits = square[...]
    ids_row[...] = jnp.zeros_like(ids_row)
    ids_row[:, pl.ds(0, rows)] = ids_ref[...]
    chosen = jnp.concatenate(
        [
            jnp.sum(
                jnp.where(below == ids_row[k : k + 1, :], logits, 0.0), axis=0, keepdims=True
            )
            for k in range(ids_row.shape[0])
        ],
        axis=0,
    )
    exps = jnp.exp(chosen - jnp.max(chosen, axis=0, keepdims=True))
    mixing = exps / jnp.sum(exps, axis=0, keepdims=True)
    lane = lax.broadcasted_iota(jnp.int32, mixing.shape, 1)
    metas[z, 0] = jnp.where(
        lane < rows, ids_row[...].astype(jnp.float32), pltpu.roll(mixing, rows, 1)
    )
    upper[...] = jnp.where(
        (below < across) & ((below >= rows) == (across >= rows)), 1.0, 0.0
    ).astype(jnp.bfloat16)

    size = block * message
    target = lax.broadcasted_iota(jnp.int32, (size, size), 0)
    source = lax.broadcasted_iota(jnp.int32, (1, size), 1)
    expert_of = lax.rem(source, block)
    perm[...] = jnp.where(
        target == expert_of * message + (source - expert_of) // block, 1.0, 0.0
    ).astype(jnp.bfloat16)
    for copy in raw:
        copy.wait()
    ordered = jnp.dot(
        perm[...], down_raw[...].reshape(size, blocks * LANES), preferred_element_type=jnp.float32
    ).astype(jnp.bfloat16)
    for g in range(blocks):
        down_out[pl.ds(g * block, block)] = ordered[:, g * LANES : (g + 1) * LANES].reshape(
            block, message, LANES
        )

    source_of = source // message
    within = source - source_of * message
    strip_of = within // down_rows
    perm[...] = jnp.where(
        target
        == strip_of * (block * down_rows) + source_of * down_rows + within - strip_of * down_rows,
        1.0,
        0.0,
    ).astype(jnp.bfloat16)

    wait_bytes(gu_stage, load_sem)
    pl.semaphore_wait(barrier, 2 * (nz - 1) + 1 + TEAM - 1)

    def gu_at(index):
        return wgu.at[index, :, columns]

    def send_gu(e, ahead, to):
        remote(gu_stage.at[e], gu_at(me), gu_send, gu_recv.at[ahead], to).start()

    def send_down(e, ahead, to):
        remote(down_out.at[e], down_in.at[quad, me], down_send, down_recv.at[ahead], to).start()

    own_gu = pltpu.make_async_copy(gu_stage.at[me], gu_at(me), own_sem.at[0])
    own_down = pltpu.make_async_copy(down_out.at[me], down_in.at[quad, me], own_sem.at[1])
    own_gu.start()
    own_down.start()

    def chip_behind(way, s):
        return lax.rem(z + (nz - s if way == 0 else s), nz)

    def ring(way, s, part):
        at = tokens.at[chip_behind(way, s - 1), 0, pl.ds(part * half, half)]
        return remote(at, at, ring_send, ring_recv.at[way, s - 1, part], towards[way])

    def ring_metas(way, s):
        at = metas.at[chip_behind(way, s - 1), 0]
        return remote(at, at, ring_meta_send, ring_meta.at[way, s - 1], towards[way])

    def wait_ring(way, s, part):
        wait_bytes(
            tokens.at[chip_behind(way, s), 0, pl.ds(part * half, half)],
            ring_recv.at[way, s - 1, part],
        )

    def wait_ring_meta(way, s):
        wait_bytes(metas.at[chip_behind(way, s), 0], ring_meta.at[way, s - 1])

    def pair_up(t, way, s):
        remote(
            tokens.at[t, 0], tokens.at[t, 1], pair_send, pair_recv.at[way, s - 1], partner
        ).start()
        remote(
            metas.at[t, 0], metas.at[t, 1], pair_meta_send, pair_meta.at[way, s - 1], partner
        ).start()

    for way in range(2):
        ring_metas(way, 1).start()
        for part in range(2):
            ring(way, 1, part).start()
    pair_up(z, 1, half_ring)
    send_down(z * 2 + 1 - core, 0, partner)
    send_gu(z * 2 + 1 - core, 0, partner)

    def share_gu(zz):
        at = wgu.at[pl.ds(zz * 2, 2), :, columns]
        for m in range(1, TEAM):
            remote(at, at, gu_fwd, gu_mate.at[m - 1], mates[m - 1]).start()

    def share_down(zz):
        at = down_in.at[quad, pl.ds(zz * 2, 2)]
        for m in range(1, TEAM):
            remote(at, at, down_fwd, down_mate.at[m - 1], mates[m - 1]).start()

    own_down.wait()
    wait_bytes(down_in.at[quad, z * 2 + 1 - core], down_recv.at[0])
    share_down(z)
    own_gu.wait()
    wait_bytes(gu_at(z * 2 + 1 - core), gu_recv.at[0])
    share_gu(z)

    def both_ways(dist, act):
        act(dist)

        @pl.when(dist < half_ring)
        def _():
            act(nz - dist)

    def issue(send):
        def act(ahead):
            zz = lax.rem(z + ahead, nz)
            for cc in range(2):
                send(zz * 2 + cc, ahead, {"z": zz, "core": cc})

        return act

    def arrived_gu(ahead):
        zz = lax.rem(z - ahead + nz, nz)
        wait_bytes(wgu.at[pl.ds(zz * 2, 2), :, columns], gu_recv.at[ahead])
        share_gu(zz)

    def arrived_down(ahead):
        zz = lax.rem(z - ahead + nz, nz)
        wait_bytes(down_in.at[quad, pl.ds(zz * 2, 2)], down_recv.at[ahead])
        share_down(zz)

    def when_step(u, late, act):
        @pl.when((u > late) & (u <= half_ring + late))
        def _():
            both_ways(half_ring + 1 + late - u, act)

    def weight_step(u):
        when_step(u, 0, issue(send_down))
        when_step(u, GU_LATE, issue(send_gu))
        when_step(u, DOWN_WAIT, arrived_down)
        when_step(u, GU_WAIT, arrived_gu)

    def attend(s):
        queries, keys, values = q_ref[s], key_ref[s], value_ref[s]
        fresh_keys = new_key_ref[s].astype(jnp.float32)
        fresh_values = new_value_ref[s].astype(jnp.float32)
        group_size = HEADS // KV_HEADS
        scale = 1.0 / math.sqrt(HEAD_DIM)
        visible = lax.broadcasted_iota(jnp.int32, (group_size, CTX), 1) < lengths_ref[s]
        for g in range(KV_HEADS):
            at = slice(g * HEAD_DIM, (g + 1) * HEAD_DIM)
            query = queries[g * group_size : (g + 1) * group_size]
            scores = scale * lax.dot_general(
                query, keys[:, at], (((1,), (1,)), ((), ())), preferred_element_type=jnp.float32
            )
            own_score = scale * jnp.sum(
                query.astype(jnp.float32) * fresh_keys[:, at], axis=1, keepdims=True
            )
            scores = jnp.where(visible, scores, -1e30)
            largest = jnp.maximum(jnp.max(scores, axis=1, keepdims=True), own_score)
            cached_exp = jnp.exp(scores - largest)
            own_exp = jnp.exp(own_score - largest)
            prob_total = jnp.sum(cached_exp, axis=1, keepdims=True) + own_exp
            cached_prob = (cached_exp / prob_total).astype(jnp.bfloat16)
            own_prob = (own_exp / prob_total).astype(jnp.bfloat16).astype(jnp.float32)
            context = jnp.dot(cached_prob, values[:, at], preferred_element_type=jnp.float32)
            context = context + own_prob * fresh_values[:, at]
            attended_ref[s, pl.ds(g * group_size, group_size), :] = context.astype(jnp.bfloat16)

    def ring_step(s, carry):
        for part in range(2):
            for way in range(2):
                if part == 0:
                    wait_ring_meta(way, s)
                    ring_metas(way, s + 1).start()
                wait_ring(way, s, part)
                ring(way, s + 1, part).start()
        for way in range(2):
            pair_up(chip_behind(way, s), way, s)
        weight_step(s)

        @pl.when(s <= q_ref.shape[0])
        def _():
            attend(s - 1)

        return carry

    lax.fori_loop(1, half_ring - 1, ring_step, 0)

    s = half_ring - 1
    for way in range(2):
        wait_ring_meta(way, s)
        if way == 0:
            ring_metas(way, s + 1).start()
        wait_ring(way, s, way)
        ring(way, s + 1, way).start()
    for way in range(2):
        wait_ring(way, s, 1 - way)
        pair_up(chip_behind(way, s), way, s)

    def weights_only(u, carry):
        weight_step(u)
        return carry

    lax.fori_loop(s, s + 1, weights_only, 0)
    s = half_ring
    wait_ring_meta(0, s)
    wait_ring(0, s, 0)
    wait_ring(1, s, 1)
    far = chip_behind(0, s)
    pair_up(far, 0, s)

    lax.fori_loop(s, half_ring + DOWN_WAIT + 1, weights_only, 0)
    for m in range(1, TEAM):
        wait_bytes(down_in.at[lax.rem(quad - m + TEAM, TEAM)], down_mate.at[m - 1])
    for g in range(blocks):
        arrived = jnp.concatenate(
            [down_in[q, pl.ds(g * block, block)].reshape(size, LANES) for q in range(TEAM)], axis=1
        )
        ordered = jnp.dot(perm[...], arrived, preferred_element_type=jnp.float32).astype(
            jnp.bfloat16
        )
        span = block * down_rows
        for c in range(strips):
            for q in range(TEAM):
                dmat[pl.ds(g * span, span), pl.ds(q * down_cut + c * LANES, LANES)] = ordered[
                    c * span : (c + 1) * span, q * LANES : (q + 1) * LANES
                ]
    lax.fori_loop(half_ring + DOWN_WAIT + 1, half_ring + GU_WAIT + 1, weights_only, 0)

    expert = me.astype(jnp.float32)

    def routing(t):
        own, other = metas[t, 0], metas[t, 1]
        lane = lax.broadcasted_iota(jnp.int32, own.shape, 1)
        ids = jnp.where(lane < rows, own, pltpu.roll(other, rows, 1))
        weights = jnp.where(lane < rows, pltpu.roll(own, rows, 1), other)
        same = ids == expert
        hit = jnp.sum(jnp.where(same, 1.0, 0.0), axis=0, keepdims=True)
        mix = jnp.sum(jnp.where(same, weights, 0.0), axis=0, keepdims=True)
        hits = jnp.broadcast_to(hit, own.shape).astype(jnp.bfloat16)
        rank = jnp.dot(hits, upper[...], preferred_element_type=jnp.float32)[0:1]
        lane = lax.broadcasted_iota(jnp.int32, (2 * SLOTS, LANES), 1)
        slot = lax.broadcasted_iota(jnp.int32, (2 * SLOTS, LANES), 0)
        rank = rank + jnp.where(lane < rows, 0.0, float(SLOTS))
        sel = jnp.where((slot.astype(jnp.float32) == rank) & (hit > 0.5), 1.0, 0.0)
        return sel, jnp.sum(sel * mix, axis=1, keepdims=True)

    def chips(s):
        return (lax.rem(z - s + nz, nz), lax.rem(z + lax.rem(s, half_ring), nz))

    def gather_part(s):
        mixes = []
        for i, t in enumerate(chips(s)):
            wait_bytes(tokens.at[t, 1], pair_recv.at[i, s - 1])
            wait_bytes(metas.at[t, 1], pair_meta.at[i, s - 1])
            sel, mix = routing(t)
            sels[i] = sel
            mixes.append(mix)
            picked[pl.ds(2 * SLOTS * i, 2 * SLOTS), :] = jnp.dot(
                sel.astype(jnp.bfloat16),
                tokens[t].reshape(2 * rows, width),
                preferred_element_type=jnp.float32,
            ).astype(jnp.bfloat16)
        return jnp.concatenate(mixes, axis=0)

    def first_part(s):
        mix = gather_part(s)
        gate_up = jnp.dot(
            picked[...], wgu[...].reshape(width, -1), preferred_element_type=jnp.float32
        )
        ff = gate_up.shape[1] // 2
        gate, up = gate_up[:, :ff], gate_up[:, ff:]
        hidden[...] = (gate / (1.0 + jnp.exp(-gate)) * up * mix).astype(jnp.bfloat16)

    def second_part(s):
        spot = lax.rem(s, 2)

        @pl.when(s < half_ring - 1)
        def _():
            wait_bytes(outgoing.at[spot], out_send.at[spot])

        rows_out = jnp.dot(hidden[...], dmat[...], preferred_element_type=jnp.float32).astype(
            jnp.bfloat16
        )
        for i, t in enumerate(chips(s)):
            spread = lax.dot_general(
                sels[i].astype(jnp.bfloat16),
                rows_out[2 * SLOTS * i : 2 * SLOTS * (i + 1)],
                (((0,), (0,)), ((), ())),
                preferred_element_type=jnp.float32,
            ).astype(jnp.bfloat16)
            outgoing[spot, i] = spread[rows:]
            mine[t] = spread[:rows]
        for i, t in enumerate(chips(s)):
            remote(
                outgoing.at[spot, i],
                theirs.at[t],
                out_send.at[spot],
                their_recv.at[i, s - 1],
                partner,
            ).start()

    def tokens_at(way, d):
        return lax.rem(z + (d if way == 0 else nz - d), nz)

    def wait_their(i, s):
        wait_bytes(theirs.at[chips(s)[i]], their_recv.at[i, s - 1])

    def onward(way, j, part):
        return remote(
            acc.at[way, j, pl.ds(part * half, half)],
            acc.at[way, j + 1, pl.ds(part * half, half)],
            sum_send,
            sum_recv.at[way, j, part],
            towards[way],
        )

    def add(way, j, t, part, fresh):
        at = pl.ds(part * half, half)
        total = mine[t, at, :].astype(jnp.float32) + theirs[t, at, :].astype(jnp.float32)
        if not fresh:
            total = total + acc[way, j, at, :].astype(jnp.float32)
        acc[way, j, at, :] = total.astype(jnp.bfloat16)

    def wait_sum(way, j, part):
        wait_bytes(acc.at[way, j, pl.ds(part * half, half)], sum_recv.at[way, j - 1, part])

    for m in range(1, TEAM):
        from_mate = lax.rem(quad - m + TEAM, TEAM)
        wait_bytes(
            wgu.at[:, :, pl.ds(pl.multiple_of(from_mate * cut, LANES), cut)], gu_mate.at[m - 1]
        )

    def sums(j, carry):
        d = half_ring - j

        @pl.when(j == 0)
        def _():
            first_part(half_ring)
            second_part(half_ring)
            wait_their(0, half_ring)
            for way in range(2):
                add(way, 0, far, way, True)
            for way in range(2):
                onward(way, 0, way).start()

        @pl.when(j == 1)
        def _():
            wait_their(0, d)
            wait_their(1, d)
            for way in range(2):
                add(way, 1, tokens_at(way, d), 1 - way, True)
            for way in range(2):
                onward(way, 1, 1 - way).start()

        @pl.when(j > 1)
        def _():
            wait_their(0, d)
            wait_their(1, d)
            for way in range(2):
                wait_sum(way, j, 0)
                add(way, j, tokens_at(way, d), 0, False)
            for way in range(2):
                onward(way, j, 0).start()

        @pl.when(d > 1)
        def _():
            first_part(d - 1)

        @pl.when(j == 1)
        def _():
            for way in range(2):
                wait_sum(way, 1, way)
                add(way, 1, tokens_at(way, d), way, False)
            for way in range(2):
                onward(way, 1, way).start()

        @pl.when(j > 1)
        def _():
            for way in range(2):
                wait_sum(way, j, 1)
                add(way, j, tokens_at(way, d), 1, False)
            for way in range(2):
                onward(way, j, 1).start()

        @pl.when(d > 1)
        def _():
            second_part(d - 1)

        return carry

    lax.fori_loop(0, half_ring, sums, 0)

    wait_their(1, half_ring)
    for part in range(2):
        at = pl.ds(part * half, half)
        for way in range(2):
            wait_sum(way, half_ring, part)
        o_ref[at, :] = (
            mine[z, at, :].astype(jnp.float32)
            + theirs[z, at, :].astype(jnp.float32)
            + acc[0, half_ring, at, :].astype(jnp.float32)
            + acc[1, half_ring, at, :].astype(jnp.float32)
        ).astype(jnp.bfloat16)

    wait_bytes(gu_stage.at[pl.ds(0, 2 * nz - 1)], gu_send)
    wait_bytes(down_out.at[pl.ds(0, 2 * nz - 1)], down_send)
    wait_bytes(wgu.at[:, :, pl.ds(0, (TEAM - 1) * cut)], gu_fwd)
    wait_bytes(down_in.at[pl.ds(0, TEAM - 1)], down_fwd)
    wait_bytes(mine.at[pl.ds(0, nz - 1)], ring_send)
    wait_bytes(metas.at[pl.ds(0, nz - 1), 0], ring_meta_send)
    wait_bytes(mine, pair_send)
    wait_bytes(metas.at[:, 0], pair_meta_send)
    wait_bytes(mine.at[pl.ds(0, nz - 1)], sum_send)
    wait_bytes(outgoing.at[0], out_send.at[0])
    wait_bytes(outgoing.at[1], out_send.at[1])


def moe(hidden_in, gain, router, ids, attention, gate, up, down, nz):
    rows, width = hidden_in.shape
    ff = gate.shape[2]
    top_count = ids.shape[0]
    down_rows = down.shape[0]
    message = down_rows * width // TEAM // LANES
    bf16 = jnp.bfloat16
    steps = nz // 2
    vmem = pltpu.VMEM
    dma = pltpu.SemaphoreType.DMA
    strips = message // down_rows
    blocks = 2 * nz // BLOCK
    here = pl.BlockSpec(memory_space=vmem)
    return pl.pallas_call(
        functools.partial(moe_kernel, nz),
        name="moe",
        out_shape=(
            jax.ShapeDtypeStruct((rows, width), bf16),
            jax.ShapeDtypeStruct(attention[0].shape, bf16),
        ),
        in_specs=[here] * 9
        + [pl.BlockSpec(memory_space=pltpu.SMEM)]
        + [pl.BlockSpec(memory_space=pl.ANY)] * 3,
        out_specs=(here, here),
        scratch_shapes=[
            vmem((nz, 2, rows, width), bf16),
            vmem((nz, 2, 8, LANES), jnp.float32),
            vmem((2 * nz, gate.shape[1], 2 * ff), bf16),
            vmem((TEAM, 2 * nz, message, LANES), bf16),
            vmem((ff, width), bf16),
            vmem((2 * nz, gate.shape[1], 2 * ff // TEAM), bf16),
            vmem((strips, down_rows, BLOCK, blocks * LANES), bf16),
            vmem((2 * nz, message, LANES), bf16),
            vmem((nz, rows, width), bf16),
            vmem((nz, rows, width), bf16),
            vmem((2, 2, rows, width), bf16),
            vmem((2, steps + 1, rows, width), bf16),
            vmem((4 * SLOTS, width), bf16),
            vmem((4 * SLOTS, ff), bf16),
            vmem((2, 2 * SLOTS, LANES), jnp.float32),
            vmem((LANES, LANES), bf16),
            vmem((BLOCK * message, BLOCK * message), bf16),
            vmem((LANES, LANES), jnp.float32),
            vmem((top_count, LANES), jnp.int32),
            dma,
            dma((strips * blocks,)),
            dma((2,)),
            dma,
            dma,
            dma,
            dma,
            dma((nz,)),
            dma((nz,)),
            dma((TEAM - 1,)),
            dma((TEAM - 1,)),
            dma,
            dma,
            dma,
            dma,
            dma((2,)),
            dma,
            dma((2, steps, 2)),
            dma((2, steps)),
            dma((2, steps)),
            dma((2, steps)),
            dma((2, steps)),
            dma((2, steps, 2)),
        ],
        compiler_params=pltpu.CompilerParams(
            collective_id=0, has_side_effects=True, vmem_limit_bytes=63 << 20
        ),
    )(hidden_in, gain, router, ids, *attention, gate, up, down)


def local(
    nz,
    queries,
    key_cache,
    value_cache,
    new_key,
    new_value,
    cache_lengths,
    hidden_in,
    norm_gain,
    router_weight,
    expert_ids,
    gate_train,
    up_train,
    down_train,
):
    seq_count = queries.shape[0]
    attention = (
        queries.reshape(seq_count, HEADS, HEAD_DIM),
        key_cache,
        value_cache,
        new_key[:, None, :],
        new_value[:, None, :],
        cache_lengths,
    )
    mixed, attended = moe(
        hidden_in,
        norm_gain[None, :],
        router_weight.T,
        expert_ids.T,
        attention,
        gate_train,
        up_train,
        jnp.swapaxes(down_train, 0, 1),
        nz,
    )
    return attended.reshape(seq_count, HEADS * HEAD_DIM), mixed


def solution(mesh):
    groups, nz = mesh.shape["groups"], mesh.shape["expert"] // 2
    torus = Mesh(mesh.devices.reshape(groups // TEAM, TEAM, nz, 2), ALL)
    placed = (
        P(ALL, None),
        P(ALL, None, None),
        P(ALL, None, None),
        P(ALL, None),
        P(ALL, None),
        P(ALL),
        P(ALL, None),
        P(),
        P(),
        P(ALL, None),
        P(None, EXPERT, None),
        P(None, EXPERT, None),
        P(None, EXPERT, None),
    )
    return jax.shard_map(
        functools.partial(local, nz),
        mesh=torus,
        in_specs=placed,
        out_specs=(P(ALL, None), P(ALL, None)),
        check_vma=False,
    )
```

```python
import functools
import math

import jax
import jax.numpy as jnp
from jax import lax
from jax.experimental import pallas as pl
from jax.experimental.pallas import tpu as pltpu
from jax.sharding import Mesh
from jax.sharding import PartitionSpec as P

HEADS = 32
KV_HEADS = 4
HEAD_DIM = 128
CTX = 64
EPSILON = 1e-06
SLOTS = 16
TEAM = 4
LANES = 128
BLOCK = 16
TAIL = 4
EARLY = 8

MESH = pl.DeviceIdType.MESH
EXPERT = ("z", "core")
ALL = ("team", "quad", "z", "core")


def rms_normed(hidden_in, norm_gain):
    values = hidden_in.astype(jnp.float32)
    mean_square = jnp.mean(values * values, axis=-1, keepdims=True)
    return (values * lax.rsqrt(mean_square + EPSILON) * norm_gain.astype(jnp.float32)).astype(
        jnp.bfloat16
    )


def remote(src, dst, send, recv, to):
    return pltpu.make_async_remote_copy(
        src_ref=src, dst_ref=dst, send_sem=send, recv_sem=recv, device_id=to, device_id_type=MESH
    )


def wait_bytes(ref, sem):
    pltpu.make_async_copy(ref, ref, sem).wait()


def moe_kernel(
    nz,
    x_ref,
    gain_ref,
    router_ref,
    ids_ref,
    q_ref,
    key_ref,
    value_ref,
    new_key_ref,
    new_value_ref,
    lengths_ref,
    gate_ref,
    up_ref,
    down_ref,
    o_ref,
    attended_ref,
    tokens,
    metas,
    wgu,
    down_in,
    dmat,
    gu_stage,
    down_raw,
    down_out,
    mine,
    theirs,
    outgoing,
    acc,
    picked,
    hidden,
    sels,
    upper,
    perm,
    square,
    ids_row,
    load_sem,
    raw_sem,
    own_sem,
    gu_send,
    down_send,
    gu_fwd,
    down_fwd,
    gu_recv,
    down_recv,
    gu_mate,
    down_mate,
    ring_send,
    ring_meta_send,
    pair_send,
    pair_meta_send,
    out_send,
    sum_send,
    ring_recv,
    ring_meta,
    pair_recv,
    pair_meta,
    their_recv,
    sum_recv,
):
    half_ring = nz // 2
    quad, z, core = lax.axis_index("quad"), lax.axis_index("z"), lax.axis_index("core")
    me = z * 2 + core
    rows, width = x_ref.shape
    half = rows // 2
    partner = {"core": 1 - core}
    after = {"z": lax.rem(z + 1, nz)}
    before = {"z": lax.rem(z + nz - 1, nz)}
    towards = (after, before)
    mates = [{"quad": lax.rem(quad + m, TEAM)} for m in range(1, TEAM)]
    cut = gu_stage.shape[2]
    columns = pl.ds(pl.multiple_of(quad * cut, LANES), cut)
    down_cut = width // TEAM
    down_rows = down_ref.shape[0]
    message = down_in.shape[2]
    strips = message // down_rows
    block = down_raw.shape[2]
    blocks = 2 * nz // block

    stage_from = pl.ds(pl.multiple_of(lax.rem(quad, TEAM // 2) * cut, LANES), cut)

    @pl.when(quad < TEAM // 2)
    def _():
        pltpu.make_async_copy(gate_ref.at[:, :, stage_from], gu_stage, load_sem).start()

    @pl.when(quad >= TEAM // 2)
    def _():
        pltpu.make_async_copy(up_ref.at[:, :, stage_from], gu_stage, load_sem).start()

    raw = []
    for c in range(strips):
        for g in range(blocks):
            at = pl.ds(pl.multiple_of(quad * down_cut + c * LANES, LANES), LANES)
            raw.append(
                pltpu.make_async_copy(
                    down_ref.at[:, pl.ds(g * block, block), at],
                    down_raw.at[c, :, :, pl.ds(g * LANES, LANES)],
                    raw_sem.at[c * blocks + g],
                )
            )
    for copy in raw:
        copy.start()

    barrier = pltpu.get_barrier_semaphore()

    def greet(i, carry):
        for cc in range(2):
            pl.semaphore_signal(
                barrier, inc=1, device_id={"z": lax.rem(z + i, nz), "core": cc}, device_id_type=MESH
            )
        return carry

    lax.fori_loop(1, nz, greet, 0)
    for who in [partner] + mates:
        pl.semaphore_signal(barrier, inc=1, device_id=who, device_id_type=MESH)

    across = lax.broadcasted_iota(jnp.int32, (LANES, LANES), 1)
    below = lax.broadcasted_iota(jnp.int32, (LANES, LANES), 0)
    normed = rms_normed(x_ref[...], gain_ref[...])
    tokens[z, 0] = normed
    square[...] = jnp.zeros_like(square)
    square[pl.ds(0, 2 * nz), pl.ds(0, rows)] = lax.dot_general(
        router_ref[...], normed, (((1,), (1,)), ((), ())), preferred_element_type=jnp.float32
    )
    logits = square[...]
    ids_row[...] = jnp.zeros_like(ids_row)
    ids_row[:, pl.ds(0, rows)] = ids_ref[...]
    chosen = jnp.concatenate(
        [
            jnp.sum(
                jnp.where(below == ids_row[k : k + 1, :], logits, 0.0), axis=0, keepdims=True
            )
            for k in range(ids_row.shape[0])
        ],
        axis=0,
    )
    exps = jnp.exp(chosen - jnp.max(chosen, axis=0, keepdims=True))
    mixing = exps / jnp.sum(exps, axis=0, keepdims=True)
    lane = lax.broadcasted_iota(jnp.int32, mixing.shape, 1)
    metas[z, 0] = jnp.where(
        lane < rows, ids_row[...].astype(jnp.float32), pltpu.roll(mixing, rows, 1)
    )
    upper[...] = jnp.where(
        (below < across) & ((below >= rows) == (across >= rows)), 1.0, 0.0
    ).astype(jnp.bfloat16)

    size = block * message
    target = lax.broadcasted_iota(jnp.int32, (size, size), 0)
    source = lax.broadcasted_iota(jnp.int32, (1, size), 1)
    expert_of = lax.rem(source, block)
    perm[...] = jnp.where(
        target == expert_of * message + (source - expert_of) // block, 1.0, 0.0
    ).astype(jnp.bfloat16)
    for copy in raw:
        copy.wait()
    ordered = jnp.dot(
        perm[...], down_raw[...].reshape(size, blocks * LANES), preferred_element_type=jnp.float32
    ).astype(jnp.bfloat16)
    for g in range(blocks):
        down_out[pl.ds(g * block, block)] = ordered[:, g * LANES : (g + 1) * LANES].reshape(
            block, message, LANES
        )

    source_of = source // message
    within = source - source_of * message
    strip_of = within // down_rows
    perm[...] = jnp.where(
        target
        == strip_of * (block * down_rows) + source_of * down_rows + within - strip_of * down_rows,
        1.0,
        0.0,
    ).astype(jnp.bfloat16)

    wait_bytes(gu_stage, load_sem)
    pl.semaphore_wait(barrier, 2 * (nz - 1) + 1 + TEAM - 1)

    def gu_at(index):
        return wgu.at[index, :, columns]

    def send_gu(e, ahead, to):
        remote(gu_stage.at[e], gu_at(me), gu_send, gu_recv.at[ahead], to).start()

    def send_down(e, ahead, to):
        remote(down_out.at[e], down_in.at[quad, me], down_send, down_recv.at[ahead], to).start()

    own_gu = pltpu.make_async_copy(gu_stage.at[me], gu_at(me), own_sem.at[0])
    own_down = pltpu.make_async_copy(down_out.at[me], down_in.at[quad, me], own_sem.at[1])
    own_gu.start()
    own_down.start()

    def chip_behind(way, s):
        return lax.rem(z + (nz - s if way == 0 else s), nz)

    def ring(way, s, part):
        at = tokens.at[chip_behind(way, s - 1), 0, pl.ds(part * half, half)]
        return remote(at, at, ring_send, ring_recv.at[way, s - 1, part], towards[way])

    def ring_metas(way, s):
        at = metas.at[chip_behind(way, s - 1), 0]
        return remote(at, at, ring_meta_send, ring_meta.at[way, s - 1], towards[way])

    def wait_ring(way, s, part):
        wait_bytes(
            tokens.at[chip_behind(way, s), 0, pl.ds(part * half, half)],
            ring_recv.at[way, s - 1, part],
        )

    def wait_ring_meta(way, s):
        wait_bytes(metas.at[chip_behind(way, s), 0], ring_meta.at[way, s - 1])

    def pair_up(t, way, s):
        remote(
            tokens.at[t, 0], tokens.at[t, 1], pair_send, pair_recv.at[way, s - 1], partner
        ).start()
        remote(
            metas.at[t, 0], metas.at[t, 1], pair_meta_send, pair_meta.at[way, s - 1], partner
        ).start()

    send_down(z * 2 + 1 - core, 0, partner)
    send_gu(z * 2 + 1 - core, 0, partner)

    def share_gu(zz):
        at = wgu.at[pl.ds(zz * 2, 2), :, columns]
        for m in range(1, TEAM):
            remote(at, at, gu_fwd, gu_mate.at[m - 1], mates[m - 1]).start()

    def share_down(zz):
        at = down_in.at[quad, pl.ds(zz * 2, 2)]
        for m in range(1, TEAM):
            remote(at, at, down_fwd, down_mate.at[m - 1], mates[m - 1]).start()

    own_down.wait()
    wait_bytes(down_in.at[quad, z * 2 + 1 - core], down_recv.at[0])
    share_down(z)
    own_gu.wait()
    wait_bytes(gu_at(z * 2 + 1 - core), gu_recv.at[0])
    share_gu(z)

    def both_ways(dist, act):
        act(dist)

        @pl.when(dist < half_ring)
        def _():
            act(nz - dist)

    def issue(send):
        def act(ahead):
            zz = lax.rem(z + ahead, nz)
            for cc in range(2):
                send(zz * 2 + cc, ahead, {"z": zz, "core": cc})

        return act

    def arrived_gu(ahead):
        zz = lax.rem(z - ahead + nz, nz)
        wait_bytes(wgu.at[pl.ds(zz * 2, 2), :, columns], gu_recv.at[ahead])
        share_gu(zz)

    def arrived_down(ahead):
        zz = lax.rem(z - ahead + nz, nz)
        wait_bytes(down_in.at[quad, pl.ds(zz * 2, 2)], down_recv.at[ahead])
        share_down(zz)

    def over_distances(first, last, act):
        def body(dist, carry):
            both_ways(dist, act)
            return carry

        lax.fori_loop(first, last + 1, body, 0)

    over_distances(1, half_ring, issue(send_down))
    over_distances(1, half_ring, issue(send_gu))
    for way in range(2):
        ring_metas(way, 1).start()
        for part in range(2):
            ring(way, 1, part).start()
    pair_up(z, 1, half_ring)

    def attend(s):
        queries, keys, values = q_ref[s], key_ref[s], value_ref[s]
        fresh_keys = new_key_ref[s].astype(jnp.float32)
        fresh_values = new_value_ref[s].astype(jnp.float32)
        group_size = HEADS // KV_HEADS
        scale = 1.0 / math.sqrt(HEAD_DIM)
        visible = lax.broadcasted_iota(jnp.int32, (group_size, CTX), 1) < lengths_ref[s]
        for g in range(KV_HEADS):
            at = slice(g * HEAD_DIM, (g + 1) * HEAD_DIM)
            query = queries[g * group_size : (g + 1) * group_size]
            scores = scale * lax.dot_general(
                query, keys[:, at], (((1,), (1,)), ((), ())), preferred_element_type=jnp.float32
            )
            own_score = scale * jnp.sum(
                query.astype(jnp.float32) * fresh_keys[:, at], axis=1, keepdims=True
            )
            scores = jnp.where(visible, scores, -1e30)
            largest = jnp.maximum(jnp.max(scores, axis=1, keepdims=True), own_score)
            cached_exp = jnp.exp(scores - largest)
            own_exp = jnp.exp(own_score - largest)
            prob_total = jnp.sum(cached_exp, axis=1, keepdims=True) + own_exp
            cached_prob = (cached_exp / prob_total).astype(jnp.bfloat16)
            own_prob = (own_exp / prob_total).astype(jnp.bfloat16).astype(jnp.float32)
            context = jnp.dot(cached_prob, values[:, at], preferred_element_type=jnp.float32)
            context = context + own_prob * fresh_values[:, at]
            attended_ref[s, pl.ds(g * group_size, group_size), :] = context.astype(jnp.bfloat16)

    over_distances(1, half_ring, arrived_down)
    over_distances(1, half_ring // 2, arrived_gu)

    def attend_one(s, carry):
        attend(s)
        return carry

    lax.fori_loop(0, q_ref.shape[0], attend_one, 0)
    for m in range(1, TEAM):
        wait_bytes(down_in.at[lax.rem(quad - m + TEAM, TEAM)], down_mate.at[m - 1])
    for g in range(blocks):
        arrived = jnp.concatenate(
            [down_in[q, pl.ds(g * block, block)].reshape(size, LANES) for q in range(TEAM)], axis=1
        )
        ordered = jnp.dot(perm[...], arrived, preferred_element_type=jnp.float32).astype(
            jnp.bfloat16
        )
        span = block * down_rows
        for c in range(strips):
            for q in range(TEAM):
                dmat[pl.ds(g * span, span), pl.ds(q * down_cut + c * LANES, LANES)] = ordered[
                    c * span : (c + 1) * span, q * LANES : (q + 1) * LANES
                ]
    over_distances(half_ring // 2 + 1, half_ring - TAIL, arrived_gu)
    expert = me.astype(jnp.float32)

    def routing(t):
        own, other = metas[t, 0], metas[t, 1]
        lane = lax.broadcasted_iota(jnp.int32, own.shape, 1)
        ids = jnp.where(lane < rows, own, pltpu.roll(other, rows, 1))
        weights = jnp.where(lane < rows, pltpu.roll(own, rows, 1), other)
        same = ids == expert
        hit = jnp.sum(jnp.where(same, 1.0, 0.0), axis=0, keepdims=True)
        mix = jnp.sum(jnp.where(same, weights, 0.0), axis=0, keepdims=True)
        hits = jnp.broadcast_to(hit, own.shape).astype(jnp.bfloat16)
        rank = jnp.dot(hits, upper[...], preferred_element_type=jnp.float32)[0:1]
        lane = lax.broadcasted_iota(jnp.int32, (2 * SLOTS, LANES), 1)
        slot = lax.broadcasted_iota(jnp.int32, (2 * SLOTS, LANES), 0)
        rank = rank + jnp.where(lane < rows, 0.0, float(SLOTS))
        sel = jnp.where((slot.astype(jnp.float32) == rank) & (hit > 0.5), 1.0, 0.0)
        return sel, jnp.sum(sel * mix, axis=1, keepdims=True)

    def chips(s):
        return (lax.rem(z - s + nz, nz), lax.rem(z + lax.rem(s, half_ring), nz))

    def gather_part(s):
        mixes = []
        for i, t in enumerate(chips(s)):
            wait_bytes(tokens.at[t, 1], pair_recv.at[i, s - 1])
            wait_bytes(metas.at[t, 1], pair_meta.at[i, s - 1])
            sel, mix = routing(t)
            sels[i] = sel
            mixes.append(mix)
            picked[pl.ds(2 * SLOTS * i, 2 * SLOTS), :] = jnp.dot(
                sel.astype(jnp.bfloat16),
                tokens[t].reshape(2 * rows, width),
                preferred_element_type=jnp.float32,
            ).astype(jnp.bfloat16)
        return jnp.concatenate(mixes, axis=0)

    def first_part(s):
        mix = gather_part(s)
        gate_up = jnp.dot(
            picked[...], wgu[...].reshape(width, -1), preferred_element_type=jnp.float32
        )
        ff = gate_up.shape[1] // 2
        gate, up = gate_up[:, :ff], gate_up[:, ff:]
        hidden[...] = (gate / (1.0 + jnp.exp(-gate)) * up * mix).astype(jnp.bfloat16)

    def second_part(s):
        spot = lax.rem(s, 2)

        @pl.when(s > 2)
        def _():
            wait_bytes(outgoing.at[spot], out_send.at[spot])

        rows_out = jnp.dot(hidden[...], dmat[...], preferred_element_type=jnp.float32).astype(
            jnp.bfloat16
        )
        for i, t in enumerate(chips(s)):
            spread = lax.dot_general(
                sels[i].astype(jnp.bfloat16),
                rows_out[2 * SLOTS * i : 2 * SLOTS * (i + 1)],
                (((0,), (0,)), ((), ())),
                preferred_element_type=jnp.float32,
            ).astype(jnp.bfloat16)
            outgoing[spot, i] = spread[rows:]
            mine[t] = spread[:rows]
        for i, t in enumerate(chips(s)):
            remote(
                outgoing.at[spot, i],
                theirs.at[t],
                out_send.at[spot],
                their_recv.at[i, s - 1],
                partner,
            ).start()

    def tokens_at(way, d):
        return lax.rem(z + (d if way == 0 else nz - d), nz)

    def wait_their(i, s):
        wait_bytes(theirs.at[chips(s)[i]], their_recv.at[i, s - 1])

    def onward(way, j, part):
        return remote(
            acc.at[way, j, pl.ds(part * half, half)],
            acc.at[way, j + 1, pl.ds(part * half, half)],
            sum_send,
            sum_recv.at[way, j, part],
            towards[way],
        )

    def add(way, j, t, part, fresh):
        at = pl.ds(part * half, half)
        total = mine[t, at, :].astype(jnp.float32) + theirs[t, at, :].astype(jnp.float32)
        if not fresh:
            total = total + acc[way, j, at, :].astype(jnp.float32)
        acc[way, j, at, :] = total.astype(jnp.bfloat16)

    def wait_sum(way, j, part):
        wait_bytes(acc.at[way, j, pl.ds(part * half, half)], sum_recv.at[way, j - 1, part])

    def ring_step(s, carry):
        chunk = s - (half_ring - 2 - EARLY)
        for part in range(2):
            for way in range(2):
                if part == 0:
                    wait_ring_meta(way, s)
                    ring_metas(way, s + 1).start()
                wait_ring(way, s, part)
                ring(way, s + 1, part).start()
            if part == 0:

                @pl.when(chunk > 0)
                def _():
                    first_part(chunk)

        for way in range(2):
            pair_up(chip_behind(way, s), way, s)

        @pl.when(chunk > 0)
        def _():
            second_part(chunk)

        @pl.when(s <= TAIL)
        def _():
            both_ways(half_ring - TAIL + s, arrived_gu)

        @pl.when(s == TAIL + 2)
        def _():
            for m in range(1, TEAM):
                from_mate = lax.rem(quad - m + TEAM, TEAM)
                wait_bytes(
                    wgu.at[:, :, pl.ds(pl.multiple_of(from_mate * cut, LANES), cut)],
                    gu_mate.at[m - 1],
                )

        return carry

    lax.fori_loop(1, half_ring - 1, ring_step, 0)

    s = half_ring - 1
    for way in range(2):
        wait_ring_meta(way, s)
        if way == 0:
            ring_metas(way, s + 1).start()
        wait_ring(way, s, way)
        ring(way, s + 1, way).start()
    for way in range(2):
        wait_ring(way, s, 1 - way)
        pair_up(chip_behind(way, s), way, s)

    s = half_ring
    wait_ring_meta(0, s)
    wait_ring(0, s, 0)
    wait_ring(1, s, 1)
    far = chip_behind(0, s)
    pair_up(far, 0, s)

    def sums(j, carry):
        d = half_ring - j

        @pl.when(j == 0)
        def _():
            first_part(half_ring)
            second_part(half_ring)
            wait_their(0, half_ring)
            for way in range(2):
                add(way, 0, far, way, True)
            for way in range(2):
                onward(way, 0, way).start()

        @pl.when(j == 1)
        def _():
            wait_their(0, d)
            wait_their(1, d)
            for way in range(2):
                add(way, 1, tokens_at(way, d), 1 - way, True)
            for way in range(2):
                onward(way, 1, 1 - way).start()

        @pl.when(j > 1)
        def _():
            wait_their(0, d)
            wait_their(1, d)
            for way in range(2):
                wait_sum(way, j, 0)
                add(way, j, tokens_at(way, d), 0, False)
            for way in range(2):
                onward(way, j, 0).start()

        @pl.when(d > EARLY + 1)
        def _():
            first_part(d - 1)

        @pl.when(j == 1)
        def _():
            for way in range(2):
                wait_sum(way, 1, way)
                add(way, 1, tokens_at(way, d), way, False)
            for way in range(2):
                onward(way, 1, way).start()

        @pl.when(j > 1)
        def _():
            for way in range(2):
                wait_sum(way, j, 1)
                add(way, j, tokens_at(way, d), 1, False)
            for way in range(2):
                onward(way, j, 1).start()

        @pl.when(d > EARLY + 1)
        def _():
            second_part(d - 1)

        return carry

    lax.fori_loop(0, half_ring, sums, 0)

    wait_their(1, half_ring)
    for part in range(2):
        at = pl.ds(part * half, half)
        for way in range(2):
            wait_sum(way, half_ring, part)
        o_ref[at, :] = (
            mine[z, at, :].astype(jnp.float32)
            + theirs[z, at, :].astype(jnp.float32)
            + acc[0, half_ring, at, :].astype(jnp.float32)
            + acc[1, half_ring, at, :].astype(jnp.float32)
        ).astype(jnp.bfloat16)

    wait_bytes(gu_stage.at[pl.ds(0, 2 * nz - 1)], gu_send)
    wait_bytes(down_out.at[pl.ds(0, 2 * nz - 1)], down_send)
    wait_bytes(wgu.at[:, :, pl.ds(0, (TEAM - 1) * cut)], gu_fwd)
    wait_bytes(down_in.at[pl.ds(0, TEAM - 1)], down_fwd)
    wait_bytes(mine.at[pl.ds(0, nz - 1)], ring_send)
    wait_bytes(metas.at[pl.ds(0, nz - 1), 0], ring_meta_send)
    wait_bytes(mine, pair_send)
    wait_bytes(metas.at[:, 0], pair_meta_send)
    wait_bytes(mine.at[pl.ds(0, nz - 1)], sum_send)
    wait_bytes(outgoing.at[0], out_send.at[0])
    wait_bytes(outgoing.at[1], out_send.at[1])


def moe(hidden_in, gain, router, ids, attention, gate, up, down, nz):
    rows, width = hidden_in.shape
    ff = gate.shape[2]
    top_count = ids.shape[0]
    down_rows = down.shape[0]
    message = down_rows * width // TEAM // LANES
    bf16 = jnp.bfloat16
    steps = nz // 2
    vmem = pltpu.VMEM
    dma = pltpu.SemaphoreType.DMA
    strips = message // down_rows
    blocks = 2 * nz // BLOCK
    here = pl.BlockSpec(memory_space=vmem)
    return pl.pallas_call(
        functools.partial(moe_kernel, nz),
        name="moe",
        out_shape=(
            jax.ShapeDtypeStruct((rows, width), bf16),
            jax.ShapeDtypeStruct(attention[0].shape, bf16),
        ),
        in_specs=[here] * 9
        + [pl.BlockSpec(memory_space=pltpu.SMEM)]
        + [pl.BlockSpec(memory_space=pl.ANY)] * 3,
        out_specs=(here, here),
        scratch_shapes=[
            vmem((nz, 2, rows, width), bf16),
            vmem((nz, 2, 8, LANES), jnp.float32),
            vmem((2 * nz, gate.shape[1], 2 * ff), bf16),
            vmem((TEAM, 2 * nz, message, LANES), bf16),
            vmem((ff, width), bf16),
            vmem((2 * nz, gate.shape[1], 2 * ff // TEAM), bf16),
            vmem((strips, down_rows, BLOCK, blocks * LANES), bf16),
            vmem((2 * nz, message, LANES), bf16),
            vmem((nz, rows, width), bf16),
            vmem((nz, rows, width), bf16),
            vmem((2, 2, rows, width), bf16),
            vmem((2, steps + 1, rows, width), bf16),
            vmem((4 * SLOTS, width), bf16),
            vmem((4 * SLOTS, ff), bf16),
            vmem((2, 2 * SLOTS, LANES), jnp.float32),
            vmem((LANES, LANES), bf16),
            vmem((BLOCK * message, BLOCK * message), bf16),
            vmem((LANES, LANES), jnp.float32),
            vmem((top_count, LANES), jnp.int32),
            dma,
            dma((strips * blocks,)),
            dma((2,)),
            dma,
            dma,
            dma,
            dma,
            dma((nz,)),
            dma((nz,)),
            dma((TEAM - 1,)),
            dma((TEAM - 1,)),
            dma,
            dma,
            dma,
            dma,
            dma((2,)),
            dma,
            dma((2, steps, 2)),
            dma((2, steps)),
            dma((2, steps)),
            dma((2, steps)),
            dma((2, steps)),
            dma((2, steps, 2)),
        ],
        compiler_params=pltpu.CompilerParams(
            collective_id=0, has_side_effects=True, vmem_limit_bytes=63 << 20
        ),
    )(hidden_in, gain, router, ids, *attention, gate, up, down)


def local(
    nz,
    queries,
    key_cache,
    value_cache,
    new_key,
    new_value,
    cache_lengths,
    hidden_in,
    norm_gain,
    router_weight,
    expert_ids,
    gate_train,
    up_train,
    down_train,
):
    seq_count = queries.shape[0]
    attention = (
        queries.reshape(seq_count, HEADS, HEAD_DIM),
        key_cache,
        value_cache,
        new_key[:, None, :],
        new_value[:, None, :],
        cache_lengths,
    )
    mixed, attended = moe(
        hidden_in,
        norm_gain[None, :],
        router_weight.T,
        expert_ids.T,
        attention,
        gate_train,
        up_train,
        jnp.swapaxes(down_train, 0, 1),
        nz,
    )
    return attended.reshape(seq_count, HEADS * HEAD_DIM), mixed


def solution(mesh):
    groups, nz = mesh.shape["groups"], mesh.shape["expert"] // 2
    torus = Mesh(mesh.devices.reshape(groups // TEAM, TEAM, nz, 2), ALL)
    placed = (
        P(ALL, None),
        P(ALL, None, None),
        P(ALL, None, None),
        P(ALL, None),
        P(ALL, None),
        P(ALL),
        P(ALL, None),
        P(),
        P(),
        P(ALL, None),
        P(None, EXPERT, None),
        P(None, EXPERT, None),
        P(None, EXPERT, None),
    )
    return jax.shard_map(
        functools.partial(local, nz),
        mesh=torus,
        in_specs=placed,
        out_specs=(P(ALL, None), P(ALL, None)),
        check_vma=False,
    )
```

```python
import functools
import math

import jax
import jax.numpy as jnp
from jax import lax
from jax.experimental import pallas as pl
from jax.experimental.pallas import tpu as pltpu
from jax.sharding import Mesh
from jax.sharding import PartitionSpec as P

HEADS = 32
KV_HEADS = 4
HEAD_DIM = 128
CTX = 64
EPSILON = 1e-06
SLOTS = 16
TEAM = 4
LANES = 128
BLOCK = 16
TAIL = 4
EARLY = 8
PIECES = 4

MESH = pl.DeviceIdType.MESH
EXPERT = ("z", "core")
ALL = ("team", "quad", "z", "core")


def rms_normed(hidden_in, norm_gain):
    values = hidden_in.astype(jnp.float32)
    mean_square = jnp.mean(values * values, axis=-1, keepdims=True)
    return (values * lax.rsqrt(mean_square + EPSILON) * norm_gain.astype(jnp.float32)).astype(
        jnp.bfloat16
    )


def remote(src, dst, send, recv, to):
    return pltpu.make_async_remote_copy(
        src_ref=src, dst_ref=dst, send_sem=send, recv_sem=recv, device_id=to, device_id_type=MESH
    )


def wait_bytes(ref, sem):
    pltpu.make_async_copy(ref, ref, sem).wait()


def moe_kernel(
    nz,
    x_ref,
    gain_ref,
    router_ref,
    ids_ref,
    q_ref,
    key_ref,
    value_ref,
    new_key_ref,
    new_value_ref,
    lengths_ref,
    gate_ref,
    up_ref,
    down_ref,
    o_ref,
    attended_ref,
    tokens,
    metas,
    wgu,
    down_in,
    dmat,
    gu_stage,
    down_raw,
    down_out,
    mine,
    theirs,
    outgoing,
    acc,
    picked,
    hidden,
    sels,
    upper,
    perm,
    square,
    ids_row,
    load_sem,
    raw_sem,
    own_sem,
    gu_send,
    down_send,
    gu_fwd,
    down_fwd,
    gu_recv,
    down_recv,
    gu_mate,
    down_mate,
    ring_send,
    ring_meta_send,
    pair_send,
    pair_meta_send,
    out_send,
    sum_send,
    ring_recv,
    ring_meta,
    pair_recv,
    pair_meta,
    their_recv,
    sum_recv,
):
    half_ring = nz // 2
    quad, z, core = lax.axis_index("quad"), lax.axis_index("z"), lax.axis_index("core")
    me = z * 2 + core
    rows, width = x_ref.shape
    piece = rows // PIECES
    halves = (range(PIECES // 2), range(PIECES // 2, PIECES))
    partner = {"core": 1 - core}
    after = {"z": lax.rem(z + 1, nz)}
    before = {"z": lax.rem(z + nz - 1, nz)}
    towards = (after, before)
    mates = [{"quad": lax.rem(quad + m, TEAM)} for m in range(1, TEAM)]
    cut = gu_stage.shape[2]
    columns = pl.ds(pl.multiple_of(quad * cut, LANES), cut)
    down_cut = width // TEAM
    down_rows = down_ref.shape[0]
    message = down_in.shape[2]
    strips = message // down_rows
    block = down_raw.shape[2]
    blocks = 2 * nz // block

    stage_from = pl.ds(pl.multiple_of(lax.rem(quad, TEAM // 2) * cut, LANES), cut)

    @pl.when(quad < TEAM // 2)
    def _():
        pltpu.make_async_copy(gate_ref.at[:, :, stage_from], gu_stage, load_sem).start()

    @pl.when(quad >= TEAM // 2)
    def _():
        pltpu.make_async_copy(up_ref.at[:, :, stage_from], gu_stage, load_sem).start()

    raw = []
    for c in range(strips):
        for g in range(blocks):
            at = pl.ds(pl.multiple_of(quad * down_cut + c * LANES, LANES), LANES)
            raw.append(
                pltpu.make_async_copy(
                    down_ref.at[:, pl.ds(g * block, block), at],
                    down_raw.at[c, :, :, pl.ds(g * LANES, LANES)],
                    raw_sem.at[c * blocks + g],
                )
            )
    for copy in raw:
        copy.start()

    barrier = pltpu.get_barrier_semaphore()

    def greet(i, carry):
        for cc in range(2):
            pl.semaphore_signal(
                barrier, inc=1, device_id={"z": lax.rem(z + i, nz), "core": cc}, device_id_type=MESH
            )
        return carry

    lax.fori_loop(1, nz, greet, 0)
    for who in [partner] + mates:
        pl.semaphore_signal(barrier, inc=1, device_id=who, device_id_type=MESH)

    across = lax.broadcasted_iota(jnp.int32, (LANES, LANES), 1)
    below = lax.broadcasted_iota(jnp.int32, (LANES, LANES), 0)
    normed = rms_normed(x_ref[...], gain_ref[...])
    tokens[z, 0] = normed
    square[...] = jnp.zeros_like(square)
    square[pl.ds(0, 2 * nz), pl.ds(0, rows)] = lax.dot_general(
        router_ref[...], normed, (((1,), (1,)), ((), ())), preferred_element_type=jnp.float32
    )
    logits = square[...]
    ids_row[...] = jnp.zeros_like(ids_row)
    ids_row[:, pl.ds(0, rows)] = ids_ref[...]
    chosen = jnp.concatenate(
        [
            jnp.sum(
                jnp.where(below == ids_row[k : k + 1, :], logits, 0.0), axis=0, keepdims=True
            )
            for k in range(ids_row.shape[0])
        ],
        axis=0,
    )
    exps = jnp.exp(chosen - jnp.max(chosen, axis=0, keepdims=True))
    mixing = exps / jnp.sum(exps, axis=0, keepdims=True)
    lane = lax.broadcasted_iota(jnp.int32, mixing.shape, 1)
    metas[z, 0] = jnp.where(
        lane < rows, ids_row[...].astype(jnp.float32), pltpu.roll(mixing, rows, 1)
    )
    upper[...] = jnp.where(
        (below < across) & ((below >= rows) == (across >= rows)), 1.0, 0.0
    ).astype(jnp.bfloat16)

    size = block * message
    target = lax.broadcasted_iota(jnp.int32, (size, size), 0)
    source = lax.broadcasted_iota(jnp.int32, (1, size), 1)
    expert_of = lax.rem(source, block)
    perm[...] = jnp.where(
        target == expert_of * message + (source - expert_of) // block, 1.0, 0.0
    ).astype(jnp.bfloat16)
    for copy in raw:
        copy.wait()
    ordered = jnp.dot(
        perm[...], down_raw[...].reshape(size, blocks * LANES), preferred_element_type=jnp.float32
    ).astype(jnp.bfloat16)
    for g in range(blocks):
        down_out[pl.ds(g * block, block)] = ordered[:, g * LANES : (g + 1) * LANES].reshape(
            block, message, LANES
        )

    source_of = source // message
    within = source - source_of * message
    strip_of = within // down_rows
    perm[...] = jnp.where(
        target
        == strip_of * (block * down_rows) + source_of * down_rows + within - strip_of * down_rows,
        1.0,
        0.0,
    ).astype(jnp.bfloat16)

    wait_bytes(gu_stage, load_sem)
    pl.semaphore_wait(barrier, 2 * (nz - 1) + 1 + TEAM - 1)

    def gu_at(index):
        return wgu.at[index, :, columns]

    def send_gu(e, ahead, to):
        remote(gu_stage.at[e], gu_at(me), gu_send, gu_recv.at[ahead], to).start()

    def send_down(e, ahead, to):
        remote(down_out.at[e], down_in.at[quad, me], down_send, down_recv.at[ahead], to).start()

    own_gu = pltpu.make_async_copy(gu_stage.at[me], gu_at(me), own_sem.at[0])
    own_down = pltpu.make_async_copy(down_out.at[me], down_in.at[quad, me], own_sem.at[1])
    own_gu.start()
    own_down.start()

    def chip_behind(way, s):
        return lax.rem(z + (nz - s if way == 0 else s), nz)

    def ring(way, s, part):
        at = tokens.at[chip_behind(way, s - 1), 0, pl.ds(part * piece, piece)]
        return remote(at, at, ring_send, ring_recv.at[way, s - 1, part], towards[way])

    def ring_metas(way, s):
        at = metas.at[chip_behind(way, s - 1), 0]
        return remote(at, at, ring_meta_send, ring_meta.at[way, s - 1], towards[way])

    def wait_ring(way, s, part):
        wait_bytes(
            tokens.at[chip_behind(way, s), 0, pl.ds(part * piece, piece)],
            ring_recv.at[way, s - 1, part],
        )

    def wait_ring_meta(way, s):
        wait_bytes(metas.at[chip_behind(way, s), 0], ring_meta.at[way, s - 1])

    def pair_up(t, way, s):
        remote(
            tokens.at[t, 0], tokens.at[t, 1], pair_send, pair_recv.at[way, s - 1], partner
        ).start()
        remote(
            metas.at[t, 0], metas.at[t, 1], pair_meta_send, pair_meta.at[way, s - 1], partner
        ).start()

    send_down(z * 2 + 1 - core, 0, partner)
    send_gu(z * 2 + 1 - core, 0, partner)

    def share_gu(zz):
        at = wgu.at[pl.ds(zz * 2, 2), :, columns]
        for m in range(1, TEAM):
            remote(at, at, gu_fwd, gu_mate.at[m - 1], mates[m - 1]).start()

    def share_down(zz):
        at = down_in.at[quad, pl.ds(zz * 2, 2)]
        for m in range(1, TEAM):
            remote(at, at, down_fwd, down_mate.at[m - 1], mates[m - 1]).start()

    own_down.wait()
    wait_bytes(down_in.at[quad, z * 2 + 1 - core], down_recv.at[0])
    share_down(z)
    own_gu.wait()
    wait_bytes(gu_at(z * 2 + 1 - core), gu_recv.at[0])
    share_gu(z)

    def both_ways(dist, act):
        act(dist)

        @pl.when(dist < half_ring)
        def _():
            act(nz - dist)

    def issue(send):
        def act(ahead):
            zz = lax.rem(z + ahead, nz)
            for cc in range(2):
                send(zz * 2 + cc, ahead, {"z": zz, "core": cc})

        return act

    def arrived_gu(ahead):
        zz = lax.rem(z - ahead + nz, nz)
        wait_bytes(wgu.at[pl.ds(zz * 2, 2), :, columns], gu_recv.at[ahead])
        share_gu(zz)

    def arrived_down(ahead):
        zz = lax.rem(z - ahead + nz, nz)
        wait_bytes(down_in.at[quad, pl.ds(zz * 2, 2)], down_recv.at[ahead])
        share_down(zz)

    def over_distances(first, last, act):
        def body(dist, carry):
            both_ways(dist, act)
            return carry

        lax.fori_loop(first, last + 1, body, 0)

    over_distances(1, half_ring, issue(send_down))
    over_distances(1, half_ring, issue(send_gu))
    for way in range(2):
        ring_metas(way, 1).start()
        for part in range(PIECES):
            ring(way, 1, part).start()
    pair_up(z, 1, half_ring)

    def attend(s):
        queries, keys, values = q_ref[s], key_ref[s], value_ref[s]
        fresh_keys = new_key_ref[s].astype(jnp.float32)
        fresh_values = new_value_ref[s].astype(jnp.float32)
        group_size = HEADS // KV_HEADS
        scale = 1.0 / math.sqrt(HEAD_DIM)
        visible = lax.broadcasted_iota(jnp.int32, (group_size, CTX), 1) < lengths_ref[s]
        for g in range(KV_HEADS):
            at = slice(g * HEAD_DIM, (g + 1) * HEAD_DIM)
            query = queries[g * group_size : (g + 1) * group_size]
            scores = scale * lax.dot_general(
                query, keys[:, at], (((1,), (1,)), ((), ())), preferred_element_type=jnp.float32
            )
            own_score = scale * jnp.sum(
                query.astype(jnp.float32) * fresh_keys[:, at], axis=1, keepdims=True
            )
            scores = jnp.where(visible, scores, -1e30)
            largest = jnp.maximum(jnp.max(scores, axis=1, keepdims=True), own_score)
            cached_exp = jnp.exp(scores - largest)
            own_exp = jnp.exp(own_score - largest)
            prob_total = jnp.sum(cached_exp, axis=1, keepdims=True) + own_exp
            cached_prob = (cached_exp / prob_total).astype(jnp.bfloat16)
            own_prob = (own_exp / prob_total).astype(jnp.bfloat16).astype(jnp.float32)
            context = jnp.dot(cached_prob, values[:, at], preferred_element_type=jnp.float32)
            context = context + own_prob * fresh_values[:, at]
            attended_ref[s, pl.ds(g * group_size, group_size), :] = context.astype(jnp.bfloat16)

    over_distances(1, half_ring, arrived_down)
    over_distances(1, half_ring // 2, arrived_gu)

    def attend_one(s, carry):
        attend(s)
        return carry

    lax.fori_loop(0, q_ref.shape[0], attend_one, 0)
    for m in range(1, TEAM):
        wait_bytes(down_in.at[lax.rem(quad - m + TEAM, TEAM)], down_mate.at[m - 1])
    for g in range(blocks):
        arrived = jnp.concatenate(
            [down_in[q, pl.ds(g * block, block)].reshape(size, LANES) for q in range(TEAM)], axis=1
        )
        ordered = jnp.dot(perm[...], arrived, preferred_element_type=jnp.float32).astype(
            jnp.bfloat16
        )
        span = block * down_rows
        for c in range(strips):
            for q in range(TEAM):
                dmat[pl.ds(g * span, span), pl.ds(q * down_cut + c * LANES, LANES)] = ordered[
                    c * span : (c + 1) * span, q * LANES : (q + 1) * LANES
                ]
    over_distances(half_ring // 2 + 1, half_ring - TAIL, arrived_gu)
    expert = me.astype(jnp.float32)

    def routing(t):
        own, other = metas[t, 0], metas[t, 1]
        lane = lax.broadcasted_iota(jnp.int32, own.shape, 1)
        ids = jnp.where(lane < rows, own, pltpu.roll(other, rows, 1))
        weights = jnp.where(lane < rows, pltpu.roll(own, rows, 1), other)
        same = ids == expert
        hit = jnp.sum(jnp.where(same, 1.0, 0.0), axis=0, keepdims=True)
        mix = jnp.sum(jnp.where(same, weights, 0.0), axis=0, keepdims=True)
        hits = jnp.broadcast_to(hit, own.shape).astype(jnp.bfloat16)
        rank = jnp.dot(hits, upper[...], preferred_element_type=jnp.float32)[0:1]
        lane = lax.broadcasted_iota(jnp.int32, (2 * SLOTS, LANES), 1)
        slot = lax.broadcasted_iota(jnp.int32, (2 * SLOTS, LANES), 0)
        rank = rank + jnp.where(lane < rows, 0.0, float(SLOTS))
        sel = jnp.where((slot.astype(jnp.float32) == rank) & (hit > 0.5), 1.0, 0.0)
        return sel, jnp.sum(sel * mix, axis=1, keepdims=True)

    def chips(s):
        return (lax.rem(z - s + nz, nz), lax.rem(z + lax.rem(s, half_ring), nz))

    def gather_part(s):
        mixes = []
        for i, t in enumerate(chips(s)):
            wait_bytes(tokens.at[t, 1], pair_recv.at[i, s - 1])
            wait_bytes(metas.at[t, 1], pair_meta.at[i, s - 1])
            sel, mix = routing(t)
            sels[i] = sel
            mixes.append(mix)
            picked[pl.ds(2 * SLOTS * i, 2 * SLOTS), :] = jnp.dot(
                sel.astype(jnp.bfloat16),
                tokens[t].reshape(2 * rows, width),
                preferred_element_type=jnp.float32,
            ).astype(jnp.bfloat16)
        return jnp.concatenate(mixes, axis=0)

    def first_part(s):
        mix = gather_part(s)
        gate_up = jnp.dot(
            picked[...], wgu[...].reshape(width, -1), preferred_element_type=jnp.float32
        )
        ff = gate_up.shape[1] // 2
        gate, up = gate_up[:, :ff], gate_up[:, ff:]
        hidden[...] = (gate / (1.0 + jnp.exp(-gate)) * up * mix).astype(jnp.bfloat16)

    def second_part(s):
        spot = lax.rem(s, 2)

        @pl.when(s > 2)
        def _():
            wait_bytes(outgoing.at[spot], out_send.at[spot])

        rows_out = jnp.dot(hidden[...], dmat[...], preferred_element_type=jnp.float32).astype(
            jnp.bfloat16
        )
        for i, t in enumerate(chips(s)):
            spread = lax.dot_general(
                sels[i].astype(jnp.bfloat16),
                rows_out[2 * SLOTS * i : 2 * SLOTS * (i + 1)],
                (((0,), (0,)), ((), ())),
                preferred_element_type=jnp.float32,
            ).astype(jnp.bfloat16)
            outgoing[spot, i] = spread[rows:]
            mine[t] = spread[:rows]
        for i, t in enumerate(chips(s)):
            remote(
                outgoing.at[spot, i],
                theirs.at[t],
                out_send.at[spot],
                their_recv.at[i, s - 1],
                partner,
            ).start()

    def tokens_at(way, d):
        return lax.rem(z + (d if way == 0 else nz - d), nz)

    def wait_their(i, s):
        wait_bytes(theirs.at[chips(s)[i]], their_recv.at[i, s - 1])

    def onward(way, j, part):
        return remote(
            acc.at[way, j, pl.ds(part * piece, piece)],
            acc.at[way, j + 1, pl.ds(part * piece, piece)],
            sum_send,
            sum_recv.at[way, j, part],
            towards[way],
        )

    def add(way, j, t, part, fresh):
        at = pl.ds(part * piece, piece)
        total = mine[t, at, :].astype(jnp.float32) + theirs[t, at, :].astype(jnp.float32)
        if not fresh:
            total = total + acc[way, j, at, :].astype(jnp.float32)
        acc[way, j, at, :] = total.astype(jnp.bfloat16)

    def wait_sum(way, j, part):
        wait_bytes(acc.at[way, j, pl.ds(part * piece, piece)], sum_recv.at[way, j - 1, part])

    def ring_step(s, carry):
        chunk = s - (half_ring - 2 - EARLY)
        for part in range(PIECES):
            for way in range(2):
                if part == 0:
                    wait_ring_meta(way, s)
                    ring_metas(way, s + 1).start()
                wait_ring(way, s, part)
                ring(way, s + 1, part).start()
            if part == PIECES // 2 - 1:

                @pl.when(chunk > 0)
                def _():
                    first_part(chunk)

        for way in range(2):
            pair_up(chip_behind(way, s), way, s)

        @pl.when(chunk > 0)
        def _():
            second_part(chunk)

        @pl.when(s <= TAIL)
        def _():
            both_ways(half_ring - TAIL + s, arrived_gu)

        @pl.when(s == TAIL + 2)
        def _():
            for m in range(1, TEAM):
                from_mate = lax.rem(quad - m + TEAM, TEAM)
                wait_bytes(
                    wgu.at[:, :, pl.ds(pl.multiple_of(from_mate * cut, LANES), cut)],
                    gu_mate.at[m - 1],
                )

        return carry

    lax.fori_loop(1, half_ring - 1, ring_step, 0)

    s = half_ring - 1
    for way in range(2):
        wait_ring_meta(way, s)
        if way == 0:
            ring_metas(way, s + 1).start()
        for part in halves[way]:
            wait_ring(way, s, part)
            ring(way, s + 1, part).start()
    for way in range(2):
        for part in halves[1 - way]:
            wait_ring(way, s, part)
        pair_up(chip_behind(way, s), way, s)

    s = half_ring
    wait_ring_meta(0, s)
    for way in range(2):
        for part in halves[way]:
            wait_ring(way, s, part)
    far = chip_behind(0, s)
    pair_up(far, 0, s)

    def sums(j, carry):
        d = half_ring - j

        @pl.when(j == 0)
        def _():
            first_part(half_ring)
            second_part(half_ring)
            wait_their(0, half_ring)
            for k in range(PIECES // 2):
                for way in range(2):
                    add(way, 0, far, halves[way][k], True)
                for way in range(2):
                    onward(way, 0, halves[way][k]).start()

        @pl.when(j > 0)
        def _():
            wait_their(0, d)
            wait_their(1, d)

        def received(part_of):
            for way in range(2):
                wait_sum(way, j, part_of[way])
                add(way, j, tokens_at(way, d), part_of[way], False)
            for way in range(2):
                onward(way, j, part_of[way]).start()

        @pl.when(j == 1)
        def _():
            for k in range(PIECES // 2):
                for way in range(2):
                    add(way, 1, tokens_at(way, d), halves[1 - way][k], True)
                for way in range(2):
                    onward(way, 1, halves[1 - way][k]).start()

        @pl.when(j > 1)
        def _():
            for part in halves[0]:
                received((part, part))

        @pl.when(d > EARLY + 1)
        def _():
            first_part(d - 1)

        @pl.when(j == 1)
        def _():
            for k in range(PIECES // 2):
                received((halves[0][k], halves[1][k]))

        @pl.when(j > 1)
        def _():
            for part in halves[1]:
                received((part, part))

        @pl.when(d > EARLY + 1)
        def _():
            second_part(d - 1)

        return carry

    lax.fori_loop(0, half_ring, sums, 0)

    wait_their(1, half_ring)
    for part in range(PIECES):
        at = pl.ds(part * piece, piece)
        for way in range(2):
            wait_sum(way, half_ring, part)
        o_ref[at, :] = (
            mine[z, at, :].astype(jnp.float32)
            + theirs[z, at, :].astype(jnp.float32)
            + acc[0, half_ring, at, :].astype(jnp.float32)
            + acc[1, half_ring, at, :].astype(jnp.float32)
        ).astype(jnp.bfloat16)

    wait_bytes(gu_stage.at[pl.ds(0, 2 * nz - 1)], gu_send)
    wait_bytes(down_out.at[pl.ds(0, 2 * nz - 1)], down_send)
    wait_bytes(wgu.at[:, :, pl.ds(0, (TEAM - 1) * cut)], gu_fwd)
    wait_bytes(down_in.at[pl.ds(0, TEAM - 1)], down_fwd)
    wait_bytes(mine.at[pl.ds(0, nz - 1)], ring_send)
    wait_bytes(metas.at[pl.ds(0, nz - 1), 0], ring_meta_send)
    wait_bytes(mine, pair_send)
    wait_bytes(metas.at[:, 0], pair_meta_send)
    wait_bytes(mine.at[pl.ds(0, nz - 1)], sum_send)
    wait_bytes(outgoing.at[0], out_send.at[0])
    wait_bytes(outgoing.at[1], out_send.at[1])


def moe(hidden_in, gain, router, ids, attention, gate, up, down, nz):
    rows, width = hidden_in.shape
    ff = gate.shape[2]
    top_count = ids.shape[0]
    down_rows = down.shape[0]
    message = down_rows * width // TEAM // LANES
    bf16 = jnp.bfloat16
    steps = nz // 2
    vmem = pltpu.VMEM
    dma = pltpu.SemaphoreType.DMA
    strips = message // down_rows
    blocks = 2 * nz // BLOCK
    here = pl.BlockSpec(memory_space=vmem)
    return pl.pallas_call(
        functools.partial(moe_kernel, nz),
        name="moe",
        out_shape=(
            jax.ShapeDtypeStruct((rows, width), bf16),
            jax.ShapeDtypeStruct(attention[0].shape, bf16),
        ),
        in_specs=[here] * 9
        + [pl.BlockSpec(memory_space=pltpu.SMEM)]
        + [pl.BlockSpec(memory_space=pl.ANY)] * 3,
        out_specs=(here, here),
        scratch_shapes=[
            vmem((nz, 2, rows, width), bf16),
            vmem((nz, 2, 8, LANES), jnp.float32),
            vmem((2 * nz, gate.shape[1], 2 * ff), bf16),
            vmem((TEAM, 2 * nz, message, LANES), bf16),
            vmem((ff, width), bf16),
            vmem((2 * nz, gate.shape[1], 2 * ff // TEAM), bf16),
            vmem((strips, down_rows, BLOCK, blocks * LANES), bf16),
            vmem((2 * nz, message, LANES), bf16),
            vmem((nz, rows, width), bf16),
            vmem((nz, rows, width), bf16),
            vmem((2, 2, rows, width), bf16),
            vmem((2, steps + 1, rows, width), bf16),
            vmem((4 * SLOTS, width), bf16),
            vmem((4 * SLOTS, ff), bf16),
            vmem((2, 2 * SLOTS, LANES), jnp.float32),
            vmem((LANES, LANES), bf16),
            vmem((BLOCK * message, BLOCK * message), bf16),
            vmem((LANES, LANES), jnp.float32),
            vmem((top_count, LANES), jnp.int32),
            dma,
            dma((strips * blocks,)),
            dma((2,)),
            dma,
            dma,
            dma,
            dma,
            dma((nz,)),
            dma((nz,)),
            dma((TEAM - 1,)),
            dma((TEAM - 1,)),
            dma,
            dma,
            dma,
            dma,
            dma((2,)),
            dma,
            dma((2, steps, PIECES)),
            dma((2, steps)),
            dma((2, steps)),
            dma((2, steps)),
            dma((2, steps)),
            dma((2, steps, PIECES)),
        ],
        compiler_params=pltpu.CompilerParams(
            collective_id=0, has_side_effects=True, vmem_limit_bytes=63 << 20
        ),
    )(hidden_in, gain, router, ids, *attention, gate, up, down)


def local(
    nz,
    queries,
    key_cache,
    value_cache,
    new_key,
    new_value,
    cache_lengths,
    hidden_in,
    norm_gain,
    router_weight,
    expert_ids,
    gate_train,
    up_train,
    down_train,
):
    seq_count = queries.shape[0]
    attention = (
        queries.reshape(seq_count, HEADS, HEAD_DIM),
        key_cache,
        value_cache,
        new_key[:, None, :],
        new_value[:, None, :],
        cache_lengths,
    )
    mixed, attended = moe(
        hidden_in,
        norm_gain[None, :],
        router_weight.T,
        expert_ids.T,
        attention,
        gate_train,
        up_train,
        jnp.swapaxes(down_train, 0, 1),
        nz,
    )
    return attended.reshape(seq_count, HEADS * HEAD_DIM), mixed


def solution(mesh):
    groups, nz = mesh.shape["groups"], mesh.shape["expert"] // 2
    torus = Mesh(mesh.devices.reshape(groups // TEAM, TEAM, nz, 2), ALL)
    placed = (
        P(ALL, None),
        P(ALL, None, None),
        P(ALL, None, None),
        P(ALL, None),
        P(ALL, None),
        P(ALL),
        P(ALL, None),
        P(),
        P(),
        P(ALL, None),
        P(None, EXPERT, None),
        P(None, EXPERT, None),
        P(None, EXPERT, None),
    )
    return jax.shard_map(
        functools.partial(local, nz),
        mesh=torus,
        in_specs=placed,
        out_specs=(P(ALL, None), P(ALL, None)),
        check_vma=False,
    )
```
